128 devices in a mesh: row: 8 (over z, core), col: 16 (over x, y).
Axes of the slice: x: 4, y: 4, z: 4, core: 2. Of those that a mesh axis runs over, the one named last changes fastest.
Arguments:
- edge_code: int32 [128, 4096], P(('row', 'col')), may hold values from 0 to 1572863
- edge_weight: bfloat16 [128, 4096], P(('row', 'col')), may hold values from 1 to 64
- edge_count: int32 [128, 128], P(('row', 'col')), may hold values from 0 to 32, as said below
- tile_blocks: int32 [128, 4, 2], P(('row', 'col')), may hold values from 0 to 127
- hub_blocks: int32 [8, 2, 2], P('row'), may hold values from 0 to 127
- node_degree: float32 [128, 512], P(('row', 'col')), may hold values from 1 to 16
Outputs:
- owned_tiles: float32 [512, 512, 512], P(('row', 'col'))
- hub_tiles: float32 [8192, 512], P(('row', 'col'))
The draws below stay inside these ranges and needn't reach their ends.
Inputs may be any that keep to these rules, and one draw needn't show every extreme that they name: `edge_count`: at most 32 used slots from one device to another; in every draw some device receives 32 used slots from every device, and the loads of destinations differ widely.
All inputs are finite; a program needn't handle non-finite values.
Results may differ from the reference program's by a relative error of at most 0.0003.
Values may be sent and summed in bfloat16 or wider, within the bound.
A program may use at most 64 MiB of HBM per device.

```python
import math
import jax
import jax.numpy as jnp
from jax import lax

TILE = 512
TILES_DEV = 4
HUBS = 2
CAP = 32
N_ROW = 8
N_COL = 16
DEVICES = 128


def draw_edge_count(key, part):
    first, second, third = jax.random.split(jax.random.fold_in(key, 7), 3)
    level = jax.random.randint(first, (1, DEVICES), 1, CAP + 1)
    counts = jax.random.randint(second, (DEVICES, DEVICES), 0, level + 1)
    target = jax.random.randint(third, (), 0, DEVICES)
    column = jnp.arange(DEVICES, dtype=jnp.int32)[None, :]
    return jnp.where(column == target, CAP, counts).astype(jnp.int32)


def with_ends(drawn, own_key, low, high):
    dims = drawn.shape
    place = [jax.random.randint(jax.random.fold_in(own_key, axis), (), 0, dims[axis]) for axis in range(len(dims))]
    drawn = drawn.at[tuple(place)].set(low)
    longest = dims.index(max(dims))
    place[longest] = (place[longest] + 1) % dims[longest]
    return drawn.at[tuple(place)].set(high)


def block_levels(stream_key, extent, cuts, least, largest):
    loudness = 1.0
    for position, shards_of in cuts:
        heights = jax.random.uniform(jax.random.fold_in(jax.random.fold_in(stream_key, 6), position), (shards_of,), jnp.float32, least / len(cuts), largest / len(cuts))
        loudness = loudness * jnp.repeat(jnp.exp(heights), extent[position] // shards_of).reshape((-1,) + (1,) * (len(extent) - 1 - position))
    return loudness


def setup_inputs(seed: int = 0) -> dict:
    arg_keys = jax.random.split(jax.random.key(seed), 7)
    return {
        "edge_code": with_ends(jax.random.randint(arg_keys[0], (DEVICES, DEVICES * CAP), 0, (TILES_DEV + HUBS) * TILE * TILE), jax.random.fold_in(arg_keys[0], 1), 0, ((TILES_DEV + HUBS) * TILE * TILE) - 1).astype(jnp.int32),
        "edge_weight": jnp.clip(jnp.exp(math.log(64.0) - 4.158883 * jax.random.uniform(arg_keys[1], (DEVICES, DEVICES * CAP), jnp.float32) ** block_levels(arg_keys[1], (DEVICES, DEVICES * CAP), ((0, 128),), -0.2, 0.2)), 1.0, 64.0).astype(jnp.bfloat16),
        "edge_count": draw_edge_count(jax.random.fold_in(arg_keys[6], 71), 0),
        "tile_blocks": with_ends(jax.random.randint(arg_keys[3], (DEVICES, TILES_DEV, 2), 0, DEVICES), jax.random.fold_in(arg_keys[3], 1), 0, DEVICES - 1).astype(jnp.int32),
        "hub_blocks": with_ends(jax.random.randint(arg_keys[4], (N_ROW, HUBS, 2), 0, DEVICES), jax.random.fold_in(arg_keys[4], 1), 0, DEVICES - 1).astype(jnp.int32),
        "node_degree": jnp.clip(jnp.exp(math.log(16.0) - 2.7725887 * jax.random.uniform(arg_keys[5], (DEVICES, TILE), jnp.float32) ** block_levels(arg_keys[5], (DEVICES, TILE), ((0, 128),), -0.2, 0.2)), 1.0, 16.0),
    }


def truncated_log(counts, row_degree, col_degree, scaling):
    return jnp.log(jnp.maximum(scaling * counts / (row_degree[..., :, None] * col_degree[..., None, :]), 1.0))


def reference(edge_code, edge_weight, edge_count, tile_blocks, hub_blocks, node_degree):
    slots = (TILES_DEV + HUBS) * TILE * TILE

    def one_device(target):
        edge_codes = lax.dynamic_slice_in_dim(edge_code, target * CAP, CAP, 1)
        weights = lax.dynamic_slice_in_dim(edge_weight, target * CAP, CAP, 1).astype(jnp.float32)
        counts = lax.dynamic_slice_in_dim(edge_count, target, 1, 1)
        usable = jnp.arange(CAP, dtype=jnp.int32)[None, :] < counts
        weights = jnp.where(usable, weights, jnp.float32(0.0))
        summed = jax.ops.segment_sum(weights.reshape(-1), edge_codes.reshape(-1).astype(jnp.int32), num_segments=slots)
        return summed.reshape(TILES_DEV + HUBS, TILE, TILE)

    totals = lax.map(one_device, jnp.arange(DEVICES, dtype=jnp.int32))
    scaling = jnp.sum(node_degree) / (DEVICES * TILE)
    owned = totals[:, :TILES_DEV].reshape(DEVICES * TILES_DEV, TILE, TILE)
    blocks = tile_blocks.reshape(DEVICES * TILES_DEV, 2)
    owned_tiles = truncated_log(owned, node_degree[blocks[:, 0]], node_degree[blocks[:, 1]], scaling)
    hubs = totals[:, TILES_DEV:].reshape(N_ROW, N_COL, HUBS, TILE, TILE).sum(axis=1)
    hub_tiles = truncated_log(hubs, node_degree[hub_blocks[:, :, 0]], node_degree[hub_blocks[:, :, 1]], scaling)
    return owned_tiles, hub_tiles.reshape(N_ROW * HUBS * TILE, TILE)
```

```python
import jax
import jax.numpy as jnp
from jax import lax
from jax.experimental import pallas as pl
from jax.experimental.pallas import tpu as pltpu
from jax.sharding import PartitionSpec as P

TILE = 512
TILES_DEV = 4
HUBS = 2
CAP = 32
N_ROW = 8
N_COL = 16
LANES = 128
CHUNK = 256
CHUNKS = TILES_DEV * TILE // CHUNK
DEPTH = 8
MESH = pl.DeviceIdType.MESH
F32 = jnp.float32
BF16 = jnp.bfloat16
NT = (((1,), (1,)), ((), ()))


def iota(shape, dim):
    return lax.broadcasted_iota(jnp.int32, shape, dim)


def exchange_kernel(
    code_ref, weight_ref, count_ref, degree_ref, slots_ref, degrees_ref,
    message, wide, row_send, row_recv, col_send, col_recv, local_sem,
):
    row = lax.axis_index("row")
    col = lax.axis_index("col")
    row_peers = [lax.rem(row + k, N_ROW) for k in range(1, N_ROW)]
    col_peers = [lax.rem(col + k, N_COL) for k in range(1, N_COL)]

    barrier = pltpu.get_barrier_semaphore()
    for peer in row_peers:
        pl.semaphore_signal(barrier, inc=1, device_id=(peer, col), device_id_type=MESH)
    for peer in col_peers:
        pl.semaphore_signal(barrier, inc=1, device_id=(row, peer), device_id_type=MESH)

    device = iota((32, LANES), 1)
    place = iota((32, LANES), 0)
    counts = jnp.where(device // 4 == place, jnp.broadcast_to(count_ref[...], (32, LANES)), 0)
    spread = (iota((LANES, LANES), 0) % 4 == iota((LANES, LANES), 1) // CAP).astype(BF16)
    counts = jnp.dot(counts.astype(BF16), spread, preferred_element_type=F32)
    for g in range(32):
        wide[pl.ds(g, 1), :] = weight_ref[:, pl.ds(g * LANES, LANES)].astype(F32)
    weights = jnp.where((device % CAP).astype(F32) < counts, wide[...], 0.0)
    for r in range(N_ROW):
        message[r, pl.ds(4, 4), :] = weights[4 * r : 4 * r + 4]
        for g in range(4):
            lanes = pl.ds((4 * r + g) * LANES, LANES)
            message[r, pl.ds(g, 1), :] = code_ref[:, lanes].astype(F32)

    pl.semaphore_wait(barrier, N_ROW + N_COL - 2)

    started = []
    for peer in row_peers:
        for part, (src, dst) in enumerate((
            (message.at[peer], slots_ref.at[col, row]),
            (degree_ref, degrees_ref.at[col, row]),
        )):
            copy = pltpu.make_async_remote_copy(
                src_ref=src, dst_ref=dst, send_sem=row_send.at[part], recv_sem=row_recv.at[part],
                device_id=(peer, col), device_id_type=MESH,
            )
            copy.start()
    own = (
        pltpu.make_async_copy(message.at[row], slots_ref.at[col, row], local_sem.at[0]),
        pltpu.make_async_copy(degree_ref, degrees_ref.at[col, row], local_sem.at[1]),
    )
    for copy in own:
        copy.start()
    for copy in own:
        copy.wait()
    others = pl.ds(0, N_ROW - 1)
    whole = (slots_ref.at[0, others], degrees_ref.at[0, others])
    for part in range(2):
        pltpu.make_async_copy(whole[part], whole[part], row_recv.at[part]).wait()

    for peer in col_peers:
        for part, ref in enumerate((slots_ref, degrees_ref)):
            pltpu.make_async_remote_copy(
                src_ref=ref.at[col], dst_ref=ref.at[col],
                send_sem=col_send.at[part], recv_sem=col_recv.at[part],
                device_id=(row, peer), device_id_type=MESH,
            ).start()
    for part in range(2):
        pltpu.make_async_copy(whole[part], whole[part], row_send.at[part]).wait()
    others = pl.ds(0, N_COL - 1)
    whole = (slots_ref.at[others], degrees_ref.at[others])
    for part in range(2):
        pltpu.make_async_copy(whole[part], whole[part], col_recv.at[part]).wait()
        pltpu.make_async_copy(whole[part], whole[part], col_send.at[part]).wait()


def exchange(code, weight, count, degree):
    vmem = pl.BlockSpec(memory_space=pltpu.VMEM)
    return pl.pallas_call(
        exchange_kernel,
        out_shape=(
            jax.ShapeDtypeStruct((N_COL, N_ROW, 8, LANES), F32),
            jax.ShapeDtypeStruct((N_COL, N_ROW, 4, LANES), F32),
        ),
        in_specs=[vmem] * 4,
        out_specs=(vmem, vmem),
        scratch_shapes=[
            pltpu.VMEM((N_ROW, 8, LANES), F32),
            pltpu.VMEM((32, LANES), F32),
            pltpu.SemaphoreType.DMA((2,)),
            pltpu.SemaphoreType.DMA((2,)),
            pltpu.SemaphoreType.DMA((2,)),
            pltpu.SemaphoreType.DMA((2,)),
            pltpu.SemaphoreType.DMA((2,)),
        ],
        compiler_params=pltpu.CompilerParams(
            collective_id=0, has_side_effects=True, vmem_limit_bytes=16 << 20
        ),
    )(code, weight, count, degree)


def one_hot(keys, rows):
    wide = jnp.broadcast_to(keys.astype(BF16), (rows, keys.shape[1]))
    return wide == iota((rows, keys.shape[1]), 0).astype(BF16)


def weighted(mask, values):
    return jnp.where(mask, jnp.broadcast_to(values.astype(BF16), mask.shape), jnp.zeros((), BF16))


def ones_where(mask):
    return jnp.where(mask, jnp.ones((), BF16), jnp.zeros((), BF16))


def two_rows(x, index):
    return jnp.concatenate([x[2 * index : 2 * index + 1], x[2 * index + 1 : 2 * index + 2]], axis=1)


def stored(block):
    return lax.rem(block, N_COL) * N_ROW + block // N_COL


def tile_kernel(
    slots_ref, degrees_ref, blocks_ref, hubs_ref, owned_ref, hub_ref,
    keys, fields, total, hub_total, staged, gathered, out_sem,
):
    col = lax.axis_index("col")

    scaling = jnp.sum(jnp.sum(degrees_ref[...], axis=0)) / (N_ROW * N_COL * TILE)
    gathered[...] = jnp.ones_like(gathered)
    for t in range(TILES_DEV):
        gathered[pl.ds(4 * t, 4), :] = degrees_ref[stored(blocks_ref[0, t, 0])]
    hub = col // 8
    hub_row = degrees_ref[stored(hubs_ref[0, hub, 0]), pl.ds(lax.rem(col, 8) // 2, 1), :]
    gathered[pl.ds(16, 8), :] = pltpu.roll(
        jnp.broadcast_to(hub_row, (8, LANES)), 64 * lax.rem(col, 2), axis=1
    )
    turned = (scaling / gathered[...]).T

    upper = iota((8, LANES), 0) < 4
    slab = 32 + col

    def collect(i, carry):
        tops, hits = carry
        first = slots_ref[pl.ds(16 * i, 8), :]
        second = slots_ref[pl.ds(16 * i + 8, 8), :]
        code = jnp.where(upper, first, pltpu.roll(second, 4, axis=0)).astype(jnp.int32)
        weight = jnp.where(upper, pltpu.roll(first, 4, axis=0), second)
        hit = jnp.logical_and(code >> 15 == slab, weight > 0.0)
        key = jnp.where(hit, ((code & 32767) << 14) + (weight * 128.0).astype(jnp.int32), 0)
        keys[pl.ds(8 * i, 8), :] = key
        kept = []
        for top in tops:
            kept.append(jnp.maximum(top, key))
            key = jnp.minimum(top, key)
        return tuple(kept), hits + hit.astype(jnp.int32)

    none = jnp.zeros((8, LANES), jnp.int32)
    tops, hits = lax.fori_loop(0, 64, collect, ((none,) * DEPTH, none), unroll=4)
    for d in range(DEPTH):
        keys[pl.ds(512 + 8 * d, 8), :] = tops[d]
    deepest = jnp.max(hits)
    fits = deepest <= DEPTH
    first_group = jnp.where(fits, 64, 0)
    groups = jnp.where(fits, deepest, 64)

    hub_total[...] = jnp.zeros_like(hub_total)

    def add_hub(i, _):
        key = keys[pl.ds(8 * (first_group + i), 8), :]
        cell = key >> 14
        weight = (key & 16383).astype(F32) * (1.0 / 128.0)
        left = ((cell >> 8) & 1) * 64 + (cell >> 9)
        left, right = left.astype(F32), (cell & 255).astype(F32)
        part = jnp.zeros((LANES, 256), F32)
        for p in range(4):
            part += lax.dot_general(
                weighted(one_hot(two_rows(left, p), LANES), two_rows(weight, p)),
                ones_where(one_hot(two_rows(right, p), 256)),
                NT, preferred_element_type=F32,
            )
        hub_total[...] += part
        return 0

    lax.fori_loop(0, groups, add_hub, 0)
    hub_degree = 1.0 / degrees_ref[stored(hubs_ref[0, hub, 1])]
    for n in range(4):
        values = hub_total[pl.ds(64 * (n // 2), 64), pl.ds(LANES * (n % 2), LANES)]
        values = values * turned[0:64, 16:17] * hub_degree[n : n + 1]
        hub_ref[:, pl.ds(LANES * n, LANES)] = jnp.log(jnp.maximum(values, 1.0))

    lane = iota((32, LANES), 1)

    def own(line):
        block = slots_ref[pl.ds(line, LANES, stride=8), :]
        joined = jnp.zeros((32, LANES), F32)
        for g in range(4):
            shift = lax.rem(CAP * g - CAP * lax.rem(col, 4) + LANES, LANES)
            part = pltpu.roll(block[32 * g : 32 * g + 32], shift, axis=1)
            joined = jnp.where(lane // CAP == g, part, joined)
        return joined

    code = own(col // 4).astype(jnp.int32)
    weight = own(4 + col // 4)
    chunk = jnp.where(weight > 0.0, code >> 17, CHUNKS)

    member = [ones_where(chunk == q) for q in range(CHUNKS)]
    member = jnp.concatenate(member, axis=0)
    upto = ones_where(iota((LANES, LANES), 0) <= iota((LANES, LANES), 1))
    inside = jnp.dot(member, upto, preferred_element_type=F32)
    lines = jnp.dot(member, jnp.ones((LANES, LANES), BF16), preferred_element_type=F32)
    before = ones_where(iota((256, 256), 1) < iota((256, 256), 0))
    base = jnp.dot(before, lines.astype(BF16), preferred_element_type=F32)
    rank = base + inside - 1.0
    place = jnp.full((32, LANES), -1.0, F32)
    for q in range(CHUNKS):
        place = jnp.where(chunk == q, rank[32 * q : 32 * q + 32], place)
    place = place.astype(jnp.int32)
    starts = [jnp.max(base[32 * q : 32 * q + 1]).astype(jnp.int32) for q in range(CHUNKS)]
    starts.append(jnp.max(base[255:256] + lines[255:256]).astype(jnp.int32))

    high, low = (place >> 7).astype(F32), (place & 127).astype(F32)
    parts = (
        (code & 255).astype(F32),
        (((code >> 8) & 1) + 2 * (code >> 17)).astype(F32),
        ((code >> 9) & 255).astype(F32),
        weight,
    )
    moved = jnp.zeros((LANES, LANES), F32)
    for p in range(16):
        mask = one_hot(two_rows(high, p), 32)
        left = jnp.concatenate([weighted(mask, two_rows(part, p)) for part in parts], axis=0)
        right = ones_where(one_hot(two_rows(low, p), LANES))
        moved += lax.dot_general(left, right, NT, preferred_element_type=F32)
    flags = moved[32:64].astype(jnp.int32)
    column = moved[0:32] + ((flags & 1) * 256).astype(F32)
    fields[0] = moved[64:96] + ((flags >> 1) * 256).astype(F32)
    fields[1] = column
    fields[2] = column - 256.0
    fields[3] = moved[96:128]

    def out_copy(q):
        return pltpu.make_async_copy(
            staged.at[q % 2], owned_ref.at[q // 2, pl.ds(CHUNK * (q % 2), CHUNK)], out_sem.at[q % 2]
        )

    for q in range(CHUNKS):
        total[...] = jnp.zeros_like(total)

        def add_block(b, _, q=q):
            def line(f):
                return jnp.concatenate(
                    [fields[f, pl.ds(2 * b, 1), :], fields[f, pl.ds(2 * b + 1, 1), :]], axis=1
                )

            left = weighted(one_hot(line(0) - 256.0 * q, CHUNK), line(3))
            right = jnp.concatenate(
                [ones_where(one_hot(line(1), 256)), ones_where(one_hot(line(2), 256))], axis=0
            )
            total[...] += lax.dot_general(left, right, NT, preferred_element_type=F32)
            return 0

        last = jnp.where(starts[q + 1] > starts[q], (starts[q + 1] + 255) >> 8, starts[q] >> 8)
        lax.fori_loop(starts[q] >> 8, last, add_block, 0)
        if q >= 2:
            out_copy(q - 2).wait()
        tile = q // 2
        degree = 1.0 / degrees_ref[stored(blocks_ref[0, tile, 1])]
        for j in range(2):
            rows = turned[:, 4 * tile + 2 * (q % 2) + j][:, None]
            for n in range(4):
                values = total[pl.ds(LANES * j, LANES), pl.ds(LANES * n, LANES)]
                values = values * rows * degree[n : n + 1]
                staged[q % 2, pl.ds(LANES * j, LANES), pl.ds(LANES * n, LANES)] = jnp.log(
                    jnp.maximum(values, 1.0)
                )
        out_copy(q).start()
    out_copy(CHUNKS - 2).wait()
    out_copy(CHUNKS - 1).wait()


def tiles(slots, degrees, blocks, hubs):
    vmem = pl.BlockSpec(memory_space=pltpu.VMEM)
    smem = pl.BlockSpec(memory_space=pltpu.SMEM)
    return pl.pallas_call(
        tile_kernel,
        out_shape=(
            jax.ShapeDtypeStruct((TILES_DEV, TILE, TILE), F32),
            jax.ShapeDtypeStruct((HUBS * TILE // N_COL, TILE), F32),
        ),
        in_specs=[vmem, vmem, smem, smem],
        out_specs=(pl.BlockSpec(memory_space=pl.ANY), vmem),
        scratch_shapes=[
            pltpu.VMEM((576, LANES), jnp.int32),
            pltpu.VMEM((4, 32, LANES), F32),
            pltpu.VMEM((CHUNK, TILE), F32),
            pltpu.VMEM((LANES, 256), F32),
            pltpu.VMEM((2, CHUNK, TILE), F32),
            pltpu.VMEM((LANES, LANES), F32),
            pltpu.SemaphoreType.DMA((2,)),
        ],
        compiler_params=pltpu.CompilerParams(vmem_limit_bytes=32 << 20),
    )(slots, degrees, blocks, hubs)


def shards(edge_code, edge_weight, edge_count, tile_blocks, hub_blocks, node_degree):
    slots, degrees = exchange(edge_code, edge_weight, edge_count, node_degree.reshape(4, LANES))
    degrees = degrees.reshape(N_COL * N_ROW, 4, LANES)
    return tiles(slots.reshape(-1, LANES), degrees, tile_blocks, hub_blocks)


def solution(mesh):
    both = ("row", "col")
    return jax.shard_map(
        shards,
        mesh=mesh,
        in_specs=(
            P(both, None), P(both, None), P(both, None),
            P(both, None, None), P("row", None, None), P(both, None),
        ),
        out_specs=(P(both, None, None), P(both, None)),
        check_vma=False,
    )
```

```python
import jax
import jax.numpy as jnp
from jax import lax
from jax.experimental import pallas as pl
from jax.experimental.pallas import tpu as pltpu
from jax.sharding import PartitionSpec as P

TILE = 512
TILES_DEV = 4
HUBS = 2
CAP = 32
N_ROW = 8
N_COL = 16
LANES = 128
CHUNK = 256
CHUNKS = TILES_DEV * TILE // CHUNK
FULL = 1 << 22
MESH = pl.DeviceIdType.MESH
F32 = jnp.float32
BF16 = jnp.bfloat16
NT = (((1,), (1,)), ((), ()))


def iota(shape, dim):
    return lax.broadcasted_iota(jnp.int32, shape, dim)


def one_hot(keys, rows):
    wide = jnp.broadcast_to(keys.astype(BF16), (rows, keys.shape[1]))
    return wide == iota((rows, keys.shape[1]), 0).astype(BF16)


def weighted(mask, values):
    return jnp.where(mask, jnp.broadcast_to(values.astype(BF16), mask.shape), jnp.zeros((), BF16))


def ones_where(mask):
    return jnp.where(mask, jnp.ones((), BF16), jnp.zeros((), BF16))


def two_rows(x, index):
    return jnp.concatenate([x[2 * index : 2 * index + 1], x[2 * index + 1 : 2 * index + 2]], axis=1)


def exchange_kernel(
    code_hbm, weight_hbm, count_hbm, degree_hbm, slots_ref, degrees_ref,
    code_ref, weight_ref, count_ref, wide, own_part, message, relay,
    in_sem, row_send, row_recv, col_send, col_recv, local_sem,
):
    row = lax.axis_index("row")
    col = lax.axis_index("col")
    row_peers = [lax.rem(row + k, N_ROW) for k in range(1, N_ROW)]
    col_peers = [lax.rem(col + k, N_COL) for k in range(1, N_COL)]

    barrier = pltpu.get_barrier_semaphore()
    for peer in col_peers:
        pl.semaphore_signal(barrier, inc=1, device_id=(row, peer), device_id_type=MESH)
    for peer in row_peers:
        pl.semaphore_signal(barrier, inc=1, device_id=(peer, col), device_id_type=MESH)
    mine = degrees_ref.at[col, row]
    inputs = [
        pltpu.make_async_copy(src, dst, in_sem.at[i])
        for i, (src, dst) in enumerate((
            (count_hbm, count_ref), (weight_hbm, weight_ref), (code_hbm, code_ref), (degree_hbm, mine),
        ))
    ]
    for copy in inputs:
        copy.start()
    for copy in inputs:
        copy.wait()

    lane = iota((32, LANES), 1)
    line = iota((32, LANES), 0)
    counts = jnp.where(lane // 4 == line, jnp.broadcast_to(count_ref[...], (32, LANES)), 0)
    spread = ones_where(iota((LANES, LANES), 0) % 4 == iota((LANES, LANES), 1) // CAP)
    counts = jnp.dot(counts.astype(BF16), spread, preferred_element_type=F32)
    for g in range(32):
        wide[pl.ds(g, 1), :] = weight_ref[:, pl.ds(g * LANES, LANES)].astype(F32)
    weights = jnp.where((lane % CAP).astype(F32) < counts, wide[...], 0.0)
    codes = code_ref[...]

    slab = jnp.where(weights > 0.0, (codes >> 15) - 32, -1)
    member = jnp.concatenate([ones_where(slab == j) for j in range(N_COL)], axis=0)
    upto = ones_where(jnp.logical_or(
        iota((LANES, 256), 0) <= iota((LANES, 256), 1), iota((LANES, 256), 1) >= LANES
    ))
    inside = jnp.dot(member, upto, preferred_element_type=F32)
    near = jnp.logical_and(
        iota((256, 256), 0) // 4 == iota((256, 256), 1) // 4, iota((256, 256), 1) < iota((256, 256), 0)
    )
    near = ones_where(near)
    rank = jnp.full((32, LANES), -1.0, F32)
    for half in range(2):
        part = inside[256 * half : 256 * half + 256]
        base = jnp.dot(near, part[:, LANES:].astype(BF16), preferred_element_type=F32)
        part = base + part[:, :LANES] - 1.0
        for j in range(8):
            rank = jnp.where(slab == 8 * half + j, part[32 * j : 32 * j + 32], rank)
    crowded = (jnp.max(rank, axis=(0, 1), keepdims=True) >= CAP).astype(F32) * FULL

    slab = slab.astype(F32)
    cell_low = (codes & 255).astype(F32)
    cell_high = ((codes >> 8) & 127).astype(F32)
    packed = []
    for r in range(N_ROW):
        part = jnp.zeros((N_COL, LANES), F32)
        for h in range(2):
            p = 2 * r + h
            mask = one_hot(two_rows(rank, p), CAP)
            none = jnp.zeros((CAP, 256), BF16)
            right = jnp.concatenate([
                weighted(mask, two_rows(cell_low, p)), none,
                weighted(mask, two_rows(cell_high, p)), weighted(mask, two_rows(weights, p)),
            ], axis=0)
            left = ones_where(one_hot(two_rows(slab, p), N_COL))
            part += lax.dot_general(left, right, NT, preferred_element_type=F32)
        packed.append(part)
    packed = jnp.concatenate(packed, axis=0)
    lanes = iota((LANES, LANES), 1)
    packed = jnp.where(lanes < 96, packed * 256.0 + pltpu.roll(packed, 64, axis=1), packed)

    flagged = codes.astype(F32) + crowded
    for u in range(4):
        left = pltpu.roll(flagged, (LANES - CAP * u) % LANES, axis=1)
        right = pltpu.roll(weights, (LANES + CAP - CAP * u) % LANES, axis=1)
        own_part[pl.ds(u, 32, stride=4), :] = jnp.where(lane < CAP, left, right)
    lines = jnp.where(lanes < 64, own_part[...], packed)
    for d in range(N_ROW * N_COL):
        message[d // N_COL, d % N_COL] = lines[d : d + 1]

    pl.semaphore_wait(barrier, N_ROW + N_COL - 2)

    def send(src, dst, send_sem, recv_sem, device):
        pltpu.make_async_remote_copy(
            src_ref=src, dst_ref=dst, send_sem=send_sem, recv_sem=recv_sem,
            device_id=device, device_id_type=MESH,
        ).start()

    for peer in row_peers:
        send(mine, mine, row_send.at[1], row_recv.at[1], (peer, col))
    for peer in row_peers:
        send(message.at[peer], relay.at[:, row], row_send.at[0], row_recv.at[0], (peer, col))
    own = pltpu.make_async_copy(message.at[row], relay.at[:, row], local_sem.at[0])
    own.start()
    own.wait()
    others = pl.ds(0, N_ROW - 1)
    rows_whole = (relay.at[:, others], degrees_ref.at[0, others])
    pltpu.make_async_copy(rows_whole[0], rows_whole[0], row_recv.at[0]).wait()
    for peer in col_peers:
        send(relay.at[peer], slots_ref.at[col], col_send.at[0], col_recv.at[0], (row, peer))
    own = pltpu.make_async_copy(relay.at[col], slots_ref.at[col], local_sem.at[1])
    own.start()
    pltpu.make_async_copy(rows_whole[1], rows_whole[1], row_recv.at[1]).wait()
    for peer in col_peers:
        send(degrees_ref.at[col], degrees_ref.at[col], col_send.at[1], col_recv.at[1], (row, peer))
    own.wait()
    others = pl.ds(0, N_COL - 1)
    cols_whole = (slots_ref.at[others], degrees_ref.at[others])
    for part in range(2):
        pltpu.make_async_copy(rows_whole[part], rows_whole[part], row_send.at[part]).wait()
    for part in range(2):
        pltpu.make_async_copy(cols_whole[part], cols_whole[part], col_send.at[part]).wait()
        pltpu.make_async_copy(cols_whole[part], cols_whole[part], col_recv.at[part]).wait()


def exchange(code, weight, count, degree):
    vmem = pl.BlockSpec(memory_space=pltpu.VMEM)
    hbm = pl.BlockSpec(memory_space=pltpu.HBM)
    pair = pltpu.SemaphoreType.DMA((2,))
    return pl.pallas_call(
        exchange_kernel,
        out_shape=(
            jax.ShapeDtypeStruct((N_COL, N_ROW, 1, LANES), F32),
            jax.ShapeDtypeStruct((N_COL, N_ROW, 4, LANES), F32),
        ),
        in_specs=[hbm] * 4,
        out_specs=(vmem, vmem),
        scratch_shapes=[
            pltpu.VMEM((32, LANES), jnp.int32),
            pltpu.VMEM((1, N_ROW * N_COL * CAP), BF16),
            pltpu.VMEM((1, LANES), jnp.int32),
            pltpu.VMEM((32, LANES), F32),
            pltpu.VMEM((LANES, LANES), F32),
            pltpu.VMEM((N_ROW, N_COL, 1, LANES), F32),
            pltpu.VMEM((N_COL, N_ROW, 1, LANES), F32),
            pltpu.SemaphoreType.DMA((4,)),
            pair, pair, pair, pair, pair,
        ],
        compiler_params=pltpu.CompilerParams(
            collective_id=0, has_side_effects=True, vmem_limit_bytes=16 << 20
        ),
    )(code, weight, count, degree)


def stored(block):
    return lax.rem(block, N_COL) * N_ROW + block // N_COL


def tile_kernel(
    slots_ref, degrees_ref, blocks_hbm, hubs_hbm, owned_ref, hub_ref, crowded_ref,
    blocks_ref, hubs_ref, hub_fields, fields, total, hub_total, staged, gathered, in_sem, out_sem,
):
    col = lax.axis_index("col")
    inputs = (
        pltpu.make_async_copy(blocks_hbm, blocks_ref, in_sem.at[0]),
        pltpu.make_async_copy(hubs_hbm, hubs_ref, in_sem.at[1]),
    )
    for copy in inputs:
        copy.start()

    turned = slots_ref[...].T
    code = turned[0:32].astype(jnp.int32)
    crowded_ref[0, 0] = (jnp.max(code) >= FULL).astype(jnp.int32)
    code = code & (FULL - 1)
    weight = turned[32:64]
    cell = turned[64:96].astype(jnp.int32)
    hub_weight = turned[96:128]
    hub_fields[0] = (((cell >> 8) & 1) * 64 + (cell >> 9)).astype(F32)
    hub_fields[1] = (cell & 255).astype(F32)
    hub_fields[2] = hub_weight
    used = jnp.max(jnp.where(hub_weight > 0.0, iota((32, LANES), 0) + 2, 0)) // 2

    chunk = jnp.where(weight > 0.0, code >> 17, CHUNKS)
    member = jnp.concatenate([ones_where(chunk == q) for q in range(CHUNKS)], axis=0)
    upto = ones_where(jnp.logical_or(
        iota((LANES, 256), 0) <= iota((LANES, 256), 1), iota((LANES, 256), 1) >= LANES
    ))
    inside = jnp.dot(member, upto, preferred_element_type=F32)
    inside, lines = inside[:, :LANES], inside[:, LANES:]
    before = ones_where(iota((256, 256), 1) < iota((256, 256), 0))
    base = jnp.dot(before, lines.astype(BF16), preferred_element_type=F32)
    rank = base + inside - 1.0
    place = jnp.full((32, LANES), -1.0, F32)
    for q in range(CHUNKS):
        place = jnp.where(chunk == q, rank[32 * q : 32 * q + 32], place)
    place = place.astype(jnp.int32)
    starts = [jnp.max(base[32 * q : 32 * q + 1]).astype(jnp.int32) for q in range(CHUNKS)]
    starts.append(jnp.max(base[255:256] + lines[255:256]).astype(jnp.int32))

    high, low = (place >> 7).astype(F32), (place & 127).astype(F32)
    parts = (
        (code & 255).astype(F32),
        (((code >> 8) & 1) + 2 * (code >> 17)).astype(F32),
        ((code >> 9) & 255).astype(F32),
        weight,
    )
    moved = jnp.zeros((LANES, LANES), F32)
    for p in range(16):
        mask = one_hot(two_rows(high, p), 32)
        left = jnp.concatenate([weighted(mask, two_rows(part, p)) for part in parts], axis=0)
        right = ones_where(one_hot(two_rows(low, p), LANES))
        moved += lax.dot_general(left, right, NT, preferred_element_type=F32)
    flags = moved[32:64].astype(jnp.int32)
    column = moved[0:32] + ((flags & 1) * 256).astype(F32)
    fields[0] = moved[64:96] + ((flags >> 1) * 256).astype(F32)
    fields[1] = column
    fields[2] = column - 256.0
    fields[3] = moved[96:128]

    scaling = jnp.sum(jnp.sum(degrees_ref[...], axis=0)) / (N_ROW * N_COL * TILE)
    for copy in inputs:
        copy.wait()
    gathered[...] = jnp.ones_like(gathered)
    for t in range(TILES_DEV):
        gathered[pl.ds(4 * t, 4), :] = degrees_ref[stored(blocks_ref[0, 0, t])]
    hub = col // 8
    hub_row = degrees_ref[stored(hubs_ref[0, hub, 0]), pl.ds(lax.rem(col, 8) // 2, 1), :]
    gathered[pl.ds(16, 8), :] = pltpu.roll(
        jnp.broadcast_to(hub_row, (8, LANES)), 64 * lax.rem(col, 2), axis=1
    )
    degree_rows = (scaling / gathered[...]).T

    def out_copy(q):
        return pltpu.make_async_copy(
            staged.at[q], owned_ref.at[q // 2, pl.ds(CHUNK * (q % 2), CHUNK)], out_sem.at[q]
        )

    for q in range(CHUNKS):
        total[...] = jnp.zeros_like(total)

        def add_block(b, _, q=q):
            def line(f):
                return jnp.concatenate(
                    [fields[f, pl.ds(2 * b, 1), :], fields[f, pl.ds(2 * b + 1, 1), :]], axis=1
                )

            left = weighted(one_hot(line(0) - 256.0 * q, CHUNK), line(3))
            right = jnp.concatenate(
                [ones_where(one_hot(line(1), 256)), ones_where(one_hot(line(2), 256))], axis=0
            )
            total[...] += lax.dot_general(left, right, NT, preferred_element_type=F32)
            return 0

        last = jnp.where(starts[q + 1] > starts[q], (starts[q + 1] + 255) >> 8, starts[q] >> 8)
        lax.fori_loop(starts[q] >> 8, last, add_block, 0)
        tile = q // 2
        degree = 1.0 / degrees_ref[stored(blocks_ref[0, 1, tile])]
        for j in range(2):
            rows = degree_rows[:, 4 * tile + 2 * (q % 2) + j][:, None]
            for n in range(4):
                values = total[pl.ds(LANES * j, LANES), pl.ds(LANES * n, LANES)]
                values = values * rows * degree[n : n + 1]
                staged[q, pl.ds(LANES * j, LANES), pl.ds(LANES * n, LANES)] = jnp.log(
                    jnp.maximum(values, 1.0)
                )
        out_copy(q).start()

    hub_total[...] = jnp.zeros_like(hub_total)

    def add_hub(b, _):
        def line(f):
            return jnp.concatenate(
                [hub_fields[f, pl.ds(2 * b, 1), :], hub_fields[f, pl.ds(2 * b + 1, 1), :]], axis=1
            )

        hub_total[...] += lax.dot_general(
            weighted(one_hot(line(0), LANES), line(2)), ones_where(one_hot(line(1), 256)),
            NT, preferred_element_type=F32,
        )
        return 0

    lax.fori_loop(0, used, add_hub, 0)
    hub_degree = 1.0 / degrees_ref[stored(hubs_ref[0, hub, 1])]
    for n in range(4):
        values = hub_total[pl.ds(64 * (n // 2), 64), pl.ds(LANES * (n % 2), LANES)]
        values = values * degree_rows[0:64, 16:17] * hub_degree[n : n + 1]
        hub_ref[:, pl.ds(LANES * n, LANES)] = jnp.log(jnp.maximum(values, 1.0))
    for q in range(CHUNKS):
        out_copy(q).wait()


def tiles(slots, degrees, blocks, hubs):
    vmem = pl.BlockSpec(memory_space=pltpu.VMEM)
    hbm = pl.BlockSpec(memory_space=pltpu.HBM)
    return pl.pallas_call(
        tile_kernel,
        out_shape=(
            jax.ShapeDtypeStruct((TILES_DEV, TILE, TILE), F32),
            jax.ShapeDtypeStruct((HUBS * TILE // N_COL, TILE), F32),
            jax.ShapeDtypeStruct((1, 1), jnp.int32),
        ),
        in_specs=[vmem, vmem, hbm, hbm],
        out_specs=(hbm, vmem, pl.BlockSpec(memory_space=pltpu.SMEM)),
        scratch_shapes=[
            pltpu.SMEM((1, 2, TILES_DEV), jnp.int32),
            pltpu.SMEM((1, HUBS, 2), jnp.int32),
            pltpu.VMEM((3, 32, LANES), F32),
            pltpu.VMEM((4, 32, LANES), F32),
            pltpu.VMEM((CHUNK, TILE), F32),
            pltpu.VMEM((LANES, 256), F32),
            pltpu.VMEM((CHUNKS, CHUNK, TILE), F32),
            pltpu.VMEM((LANES, LANES), F32),
            pltpu.SemaphoreType.DMA((2,)),
            pltpu.SemaphoreType.DMA((CHUNKS,)),
        ],
        compiler_params=pltpu.CompilerParams(vmem_limit_bytes=32 << 20),
    )(slots, degrees, blocks, hubs)


def dense_hub(code, weight, count, hubs, degrees):
    def to_owner(x):
        return lax.all_to_all(
            x.reshape(N_ROW * N_COL, -1), ("row", "col"), split_axis=0, concat_axis=0, tiled=True
        )

    codes, weights, counts = to_owner(code), to_owner(weight), to_owner(count)
    usable = jnp.arange(CAP, dtype=jnp.int32)[None, :] < counts
    weights = jnp.where(usable, weights, jnp.zeros((), BF16)).reshape(-1)
    codes = codes.reshape(-1) - TILES_DEV * TILE * TILE

    def step(turn, sums):
        part = lax.dynamic_slice_in_dim(codes, turn * 512, 512)
        value = lax.dynamic_slice_in_dim(weights, turn * 512, 512)
        left = jnp.where(
            (part >> 9)[:, None] == jnp.arange(HUBS * TILE, dtype=jnp.int32)[None, :],
            value[:, None], jnp.zeros((), BF16),
        )
        right = ((part & 511)[:, None] == jnp.arange(TILE, dtype=jnp.int32)[None, :]).astype(BF16)
        return sums + lax.dot_general(
            left, right, (((0,), (0,)), ((), ())), preferred_element_type=F32
        )

    sums = lax.fori_loop(
        0, codes.shape[0] // 512, step, jnp.zeros((HUBS * TILE, TILE), F32)
    )
    sums = sums.reshape(N_COL, HUBS * TILE // N_COL, TILE)
    sums = jnp.sum(lax.all_to_all(sums, "col", 0, 0, tiled=True), axis=0)
    slab_rows = HUBS * TILE // N_COL
    offset = lax.axis_index("col") * slab_rows
    degrees = degrees.reshape(N_ROW * N_COL, TILE)
    scaling = jnp.mean(degrees)
    pair = lax.dynamic_index_in_dim(hubs[0], offset // TILE, 0, keepdims=False)
    row_degree = lax.dynamic_index_in_dim(degrees, stored(pair[0]), 0, keepdims=False)
    row_degree = lax.dynamic_slice_in_dim(row_degree, lax.rem(offset, TILE), slab_rows)
    col_degree = lax.dynamic_index_in_dim(degrees, stored(pair[1]), 0, keepdims=False)
    return jnp.log(
        jnp.maximum(scaling * sums / (row_degree[:, None] * col_degree[None, :]), 1.0)
    )


def shards(edge_code, edge_weight, edge_count, tile_blocks, hub_blocks, node_degree):
    slots, degrees = exchange(
        edge_code.reshape(32, LANES), edge_weight, edge_count, node_degree.reshape(4, LANES)
    )
    degrees = degrees.reshape(N_COL * N_ROW, 4, LANES)
    owned, hub, crowded = tiles(
        slots.reshape(-1, LANES), degrees, tile_blocks.transpose(0, 2, 1), hub_blocks
    )
    hub = lax.cond(
        crowded[0, 0] > 0,
        lambda: dense_hub(edge_code, edge_weight, edge_count, hub_blocks, degrees),
        lambda: hub,
    )
    return owned, hub


def solution(mesh):
    both = ("row", "col")
    return jax.shard_map(
        shards,
        mesh=mesh,
        in_specs=(
            P(both, None), P(both, None), P(both, None),
            P(both, None, None), P("row", None, None), P(both, None),
        ),
        out_specs=(P(both, None, None), P(both, None)),
        check_vma=False,
    )
```

```python
import jax
import jax.numpy as jnp
from jax import lax
from jax.experimental import pallas as pl
from jax.experimental.pallas import tpu as pltpu
from jax.sharding import PartitionSpec as P

TILE = 512
TILES_DEV = 4
HUBS = 2
CAP = 32
N_ROW = 8
N_COL = 16
LANES = 128
CHUNK = 256
CHUNKS = TILES_DEV * TILE // CHUNK
FULL = 1 << 22
MESH = pl.DeviceIdType.MESH
F32 = jnp.float32
BF16 = jnp.bfloat16
NT = (((1,), (1,)), ((), ()))


def iota(shape, dim):
    return lax.broadcasted_iota(jnp.int32, shape, dim)


def one_hot(keys, rows):
    wide = jnp.broadcast_to(keys.astype(BF16), (rows, keys.shape[1]))
    return wide == iota((rows, keys.shape[1]), 0).astype(BF16)


def weighted(mask, values):
    return jnp.where(mask, jnp.broadcast_to(values.astype(BF16), mask.shape), jnp.zeros((), BF16))


def ones_where(mask):
    return jnp.where(mask, jnp.ones((), BF16), jnp.zeros((), BF16))


def two_rows(x, index):
    return jnp.concatenate([x[2 * index : 2 * index + 1], x[2 * index + 1 : 2 * index + 2]], axis=1)


def exchange_kernel(
    code_hbm, weight_hbm, count_hbm, degree_hbm, slots_ref, degrees_ref,
    code_ref, weight_ref, count_ref, wide, own_part, message, relay,
    in_sem, row_send, row_recv, col_send, col_recv, local_sem,
):
    row = lax.axis_index("row")
    col = lax.axis_index("col")
    row_peers = [lax.rem(row + k, N_ROW) for k in range(1, N_ROW)]
    col_peers = [lax.rem(col + k, N_COL) for k in range(1, N_COL)]

    barrier = pltpu.get_barrier_semaphore()
    for peer in col_peers:
        pl.semaphore_signal(barrier, inc=1, device_id=(row, peer), device_id_type=MESH)
    for peer in row_peers:
        pl.semaphore_signal(barrier, inc=1, device_id=(peer, col), device_id_type=MESH)
    mine = degrees_ref.at[col, row]
    inputs = [
        pltpu.make_async_copy(src, dst, in_sem.at[i])
        for i, (src, dst) in enumerate((
            (count_hbm, count_ref), (weight_hbm, weight_ref), (code_hbm, code_ref), (degree_hbm, mine),
        ))
    ]
    for copy in inputs:
        copy.start()
    for copy in inputs:
        copy.wait()

    lane = iota((32, LANES), 1)
    line = iota((32, LANES), 0)
    counts = jnp.where(lane // 4 == line, jnp.broadcast_to(count_ref[...], (32, LANES)), 0)
    spread = ones_where(iota((LANES, LANES), 0) % 4 == iota((LANES, LANES), 1) // CAP)
    counts = jnp.dot(counts.astype(BF16), spread, preferred_element_type=F32)
    for g in range(32):
        wide[pl.ds(g, 1), :] = weight_ref[:, pl.ds(g * LANES, LANES)].astype(F32)
    weights = jnp.where((lane % CAP).astype(F32) < counts, wide[...], 0.0)
    codes = code_ref[...]

    slab = jnp.where(weights > 0.0, (codes >> 15) - 32, -1)
    member = jnp.concatenate([ones_where(slab == j) for j in range(N_COL)], axis=0)
    upto = ones_where(jnp.logical_or(
        iota((LANES, 256), 0) <= iota((LANES, 256), 1), iota((LANES, 256), 1) >= LANES
    ))
    inside = jnp.dot(member, upto, preferred_element_type=F32)
    near = jnp.logical_and(
        iota((256, 256), 0) // 4 == iota((256, 256), 1) // 4, iota((256, 256), 1) < iota((256, 256), 0)
    )
    near = ones_where(near)
    rank = jnp.full((32, LANES), -1.0, F32)
    for half in range(2):
        part = inside[256 * half : 256 * half + 256]
        base = jnp.dot(near, part[:, LANES:].astype(BF16), preferred_element_type=F32)
        part = base + part[:, :LANES] - 1.0
        for j in range(8):
            rank = jnp.where(slab == 8 * half + j, part[32 * j : 32 * j + 32], rank)
    crowded = (jnp.max(rank, axis=(0, 1), keepdims=True) >= CAP).astype(F32) * FULL

    slab = slab.astype(F32)
    cell_low = (codes & 255).astype(F32)
    cell_high = ((codes >> 8) & 127).astype(F32)
    packed = []
    for r in range(N_ROW):
        part = jnp.zeros((N_COL, LANES), F32)
        for h in range(2):
            p = 2 * r + h
            mask = one_hot(two_rows(rank, p), CAP)
            none = jnp.zeros((CAP, 256), BF16)
            right = jnp.concatenate([
                weighted(mask, two_rows(cell_low, p)), none,
                weighted(mask, two_rows(cell_high, p)), weighted(mask, two_rows(weights, p)),
            ], axis=0)
            left = ones_where(one_hot(two_rows(slab, p), N_COL))
            part += lax.dot_general(left, right, NT, preferred_element_type=F32)
        packed.append(part)
    packed = jnp.concatenate(packed, axis=0)
    lanes = iota((LANES, LANES), 1)
    packed = jnp.where(lanes < 96, packed * 256.0 + pltpu.roll(packed, 64, axis=1), packed)

    flagged = codes.astype(F32) + crowded
    for u in range(4):
        left = pltpu.roll(flagged, (LANES - CAP * u) % LANES, axis=1)
        right = pltpu.roll(weights, (LANES + CAP - CAP * u) % LANES, axis=1)
        own_part[pl.ds(u, 32, stride=4), :] = jnp.where(lane < CAP, left, right)
    lines = jnp.where(lanes < 64, own_part[...], packed)
    for d in range(N_ROW * N_COL):
        message[d // N_COL, d % N_COL] = lines[d : d + 1]

    pl.semaphore_wait(barrier, N_ROW + N_COL - 2)

    def send(src, dst, send_sem, recv_sem, device):
        pltpu.make_async_remote_copy(
            src_ref=src, dst_ref=dst, send_sem=send_sem, recv_sem=recv_sem,
            device_id=device, device_id_type=MESH,
        ).start()

    for peer in row_peers:
        send(mine, mine, row_send.at[1], row_recv.at[1], (peer, col))
    for peer in row_peers:
        send(message.at[peer], relay.at[:, row], row_send.at[0], row_recv.at[0], (peer, col))
    own = pltpu.make_async_copy(message.at[row], relay.at[:, row], local_sem.at[0])
    own.start()
    own.wait()
    others = pl.ds(0, N_ROW - 1)
    rows_whole = (relay.at[:, others], degrees_ref.at[0, others])
    pltpu.make_async_copy(rows_whole[0], rows_whole[0], row_recv.at[0]).wait()
    for peer in col_peers:
        send(relay.at[peer], slots_ref.at[col], col_send.at[0], col_recv.at[0], (row, peer))
    own = pltpu.make_async_copy(relay.at[col], slots_ref.at[col], local_sem.at[1])
    own.start()
    pltpu.make_async_copy(rows_whole[1], rows_whole[1], row_recv.at[1]).wait()
    for peer in col_peers:
        send(degrees_ref.at[col], degrees_ref.at[col], col_send.at[1], col_recv.at[1], (row, peer))
    own.wait()
    others = pl.ds(0, N_COL - 1)
    cols_whole = (slots_ref.at[others], degrees_ref.at[others])
    for part in range(2):
        pltpu.make_async_copy(rows_whole[part], rows_whole[part], row_send.at[part]).wait()
    for part in range(2):
        pltpu.make_async_copy(cols_whole[part], cols_whole[part], col_send.at[part]).wait()
        pltpu.make_async_copy(cols_whole[part], cols_whole[part], col_recv.at[part]).wait()


def exchange(code, weight, count, degree):
    vmem = pl.BlockSpec(memory_space=pltpu.VMEM)
    hbm = pl.BlockSpec(memory_space=pltpu.HBM)
    pair = pltpu.SemaphoreType.DMA((2,))
    return pl.pallas_call(
        exchange_kernel,
        out_shape=(
            jax.ShapeDtypeStruct((N_COL, N_ROW, 1, LANES), F32),
            jax.ShapeDtypeStruct((N_COL, N_ROW, 4, LANES), F32),
        ),
        in_specs=[hbm] * 4,
        out_specs=(vmem, vmem),
        scratch_shapes=[
            pltpu.VMEM((32, LANES), jnp.int32),
            pltpu.VMEM((1, N_ROW * N_COL * CAP), BF16),
            pltpu.VMEM((1, LANES), jnp.int32),
            pltpu.VMEM((32, LANES), F32),
            pltpu.VMEM((LANES, LANES), F32),
            pltpu.VMEM((N_ROW, N_COL, 1, LANES), F32),
            pltpu.VMEM((N_COL, N_ROW, 1, LANES), F32),
            pltpu.SemaphoreType.DMA((4,)),
            pair, pair, pair, pair, pair,
        ],
        compiler_params=pltpu.CompilerParams(
            collective_id=0, has_side_effects=True, vmem_limit_bytes=16 << 20
        ),
    )(code, weight, count, degree)


def stored(block):
    return lax.rem(block, N_COL) * N_ROW + block // N_COL


def tile_kernel(
    slots_ref, degrees_ref, blocks_hbm, hubs_hbm, owned_ref, hub_out, crowded_out,
    blocks_ref, hubs_ref, crowded_ref, hub_fields, fields, total, hub_total, staged, hub_ref, gathered,
    in_sem, out_sem, flag_sem,
):
    col = lax.axis_index("col")
    inputs = (
        pltpu.make_async_copy(blocks_hbm, blocks_ref, in_sem.at[0]),
        pltpu.make_async_copy(hubs_hbm, hubs_ref, in_sem.at[1]),
    )
    for copy in inputs:
        copy.start()

    turned = slots_ref[...].T
    code = turned[0:32].astype(jnp.int32)
    crowded_ref[0, 0] = (jnp.max(code) >= FULL).astype(jnp.int32)
    flag_copy = pltpu.make_async_copy(crowded_ref, crowded_out, flag_sem)
    flag_copy.start()
    code = code & (FULL - 1)
    weight = turned[32:64]
    cell = turned[64:96].astype(jnp.int32)
    hub_weight = turned[96:128]
    hub_fields[0] = (((cell >> 8) & 1) * 64 + (cell >> 9)).astype(F32)
    hub_fields[1] = (cell & 255).astype(F32)
    hub_fields[2] = hub_weight
    used = jnp.max(jnp.where(hub_weight > 0.0, iota((32, LANES), 0) + 2, 0)) // 2

    chunk = jnp.where(weight > 0.0, code >> 17, CHUNKS)
    member = jnp.concatenate([ones_where(chunk == q) for q in range(CHUNKS)], axis=0)
    upto = ones_where(jnp.logical_or(
        iota((LANES, 256), 0) <= iota((LANES, 256), 1), iota((LANES, 256), 1) >= LANES
    ))
    inside = jnp.dot(member, upto, preferred_element_type=F32)
    inside, lines = inside[:, :LANES], inside[:, LANES:]
    before = ones_where(iota((256, 256), 1) < iota((256, 256), 0))
    base = jnp.dot(before, lines.astype(BF16), preferred_element_type=F32)
    rank = base + inside - 1.0
    place = jnp.full((32, LANES), -1.0, F32)
    for q in range(CHUNKS):
        place = jnp.where(chunk == q, rank[32 * q : 32 * q + 32], place)
    place = place.astype(jnp.int32)
    starts = [jnp.max(base[32 * q : 32 * q + 1]).astype(jnp.int32) for q in range(CHUNKS)]
    starts.append(jnp.max(base[255:256] + lines[255:256]).astype(jnp.int32))

    high, low = (place >> 7).astype(F32), (place & 127).astype(F32)
    parts = (
        (code & 255).astype(F32),
        (((code >> 8) & 1) + 2 * (code >> 17)).astype(F32),
        ((code >> 9) & 255).astype(F32),
        weight,
    )
    moved = jnp.zeros((LANES, LANES), F32)
    for p in range(16):
        mask = one_hot(two_rows(high, p), 32)
        left = jnp.concatenate([weighted(mask, two_rows(part, p)) for part in parts], axis=0)
        right = ones_where(one_hot(two_rows(low, p), LANES))
        moved += lax.dot_general(left, right, NT, preferred_element_type=F32)
    flags = moved[32:64].astype(jnp.int32)
    column = moved[0:32] + ((flags & 1) * 256).astype(F32)
    fields[0] = moved[64:96] + ((flags >> 1) * 256).astype(F32)
    fields[1] = column
    fields[2] = column - 256.0
    fields[3] = moved[96:128]

    def out_copy(q):
        return pltpu.make_async_copy(
            staged.at[q], owned_ref.at[q // 2, pl.ds(CHUNK * (q % 2), CHUNK)], out_sem.at[q]
        )

    def product(b, q):
        def line(f):
            return jnp.concatenate(
                [fields[f, pl.ds(2 * b, 1), :], fields[f, pl.ds(2 * b + 1, 1), :]], axis=1
            )

        left = weighted(one_hot(line(0) - 256.0 * q, CHUNK), line(3))
        right = jnp.concatenate(
            [ones_where(one_hot(line(1), 256)), ones_where(one_hot(line(2), 256))], axis=0
        )
        return lax.dot_general(left, right, NT, preferred_element_type=F32)

    firsts = [jnp.minimum(starts[q] >> 8, 15) for q in range(CHUNKS)]

    def add_rest(q):
        def add_block(b, _):
            total[q % 2] += product(b, q)
            return 0

        last = jnp.where(starts[q + 1] > starts[q], (starts[q + 1] + 255) >> 8, 0)
        lax.fori_loop(firsts[q] + 1, last, add_block, 0)

    total[0] = product(firsts[0], 0)
    add_rest(0)

    scaling = jnp.sum(jnp.sum(degrees_ref[...], axis=0)) / (N_ROW * N_COL * TILE)
    for copy in inputs:
        copy.wait()
    gathered[...] = jnp.ones_like(gathered)
    for t in range(TILES_DEV):
        gathered[pl.ds(4 * t, 4), :] = degrees_ref[stored(blocks_ref[0, 0, t])]
    hub = col // 8
    hub_row = degrees_ref[stored(hubs_ref[0, hub, 0]), pl.ds(lax.rem(col, 8) // 2, 1), :]
    gathered[pl.ds(16, 8), :] = pltpu.roll(
        jnp.broadcast_to(hub_row, (8, LANES)), 64 * lax.rem(col, 2), axis=1
    )
    degree_rows = (scaling / gathered[...]).T

    for q in range(CHUNKS):
        if q + 1 < CHUNKS:
            total[(q + 1) % 2] = product(firsts[q + 1], q + 1)
        tile = q // 2
        degree = 1.0 / degrees_ref[stored(blocks_ref[0, 1, tile])]
        for j in range(2):
            rows = degree_rows[:, 4 * tile + 2 * (q % 2) + j][:, None]
            for n in range(4):
                values = total[q % 2, pl.ds(LANES * j, LANES), pl.ds(LANES * n, LANES)]
                values = values * rows * degree[n : n + 1]
                staged[q, pl.ds(LANES * j, LANES), pl.ds(LANES * n, LANES)] = jnp.log(
                    jnp.maximum(values, 1.0)
                )
        out_copy(q).start()
        if q + 1 < CHUNKS:
            add_rest(q + 1)

    hub_total[...] = jnp.zeros_like(hub_total)

    def add_hub(b, _):
        def line(f):
            return jnp.concatenate(
                [hub_fields[f, pl.ds(2 * b, 1), :], hub_fields[f, pl.ds(2 * b + 1, 1), :]], axis=1
            )

        hub_total[...] += lax.dot_general(
            weighted(one_hot(line(0), LANES), line(2)), ones_where(one_hot(line(1), 256)),
            NT, preferred_element_type=F32,
        )
        return 0

    lax.fori_loop(0, used, add_hub, 0)
    hub_degree = 1.0 / degrees_ref[stored(hubs_ref[0, hub, 1])]
    for n in range(4):
        values = hub_total[pl.ds(64 * (n // 2), 64), pl.ds(LANES * (n % 2), LANES)]
        values = values * degree_rows[0:64, 16:17] * hub_degree[n : n + 1]
        hub_ref[:, pl.ds(LANES * n, LANES)] = jnp.log(jnp.maximum(values, 1.0))
    hub_copy = pltpu.make_async_copy(hub_ref, hub_out, out_sem.at[CHUNKS])
    hub_copy.start()
    flag_copy.wait()
    hub_copy.wait()
    for q in range(CHUNKS):
        out_copy(q).wait()


def tiles(slots, degrees, blocks, hubs):
    vmem = pl.BlockSpec(memory_space=pltpu.VMEM)
    hbm = pl.BlockSpec(memory_space=pltpu.HBM)
    return pl.pallas_call(
        tile_kernel,
        out_shape=(
            jax.ShapeDtypeStruct((TILES_DEV, TILE, TILE), F32),
            jax.ShapeDtypeStruct((HUBS * TILE // N_COL, TILE), F32),
            jax.ShapeDtypeStruct((1, 1), jnp.int32),
        ),
        in_specs=[vmem, vmem, hbm, hbm],
        out_specs=(hbm, hbm, hbm),
        scratch_shapes=[
            pltpu.SMEM((1, 2, TILES_DEV), jnp.int32),
            pltpu.SMEM((1, HUBS, 2), jnp.int32),
            pltpu.SMEM((1, 1), jnp.int32),
            pltpu.VMEM((3, 32, LANES), F32),
            pltpu.VMEM((4, 32, LANES), F32),
            pltpu.VMEM((2, CHUNK, TILE), F32),
            pltpu.VMEM((LANES, 256), F32),
            pltpu.VMEM((CHUNKS, CHUNK, TILE), F32),
            pltpu.VMEM((HUBS * TILE // N_COL, TILE), F32),
            pltpu.VMEM((LANES, LANES), F32),
            pltpu.SemaphoreType.DMA((2,)),
            pltpu.SemaphoreType.DMA((CHUNKS + 1,)),
            pltpu.SemaphoreType.DMA(()),
        ],
        compiler_params=pltpu.CompilerParams(vmem_limit_bytes=32 << 20),
    )(slots, degrees, blocks, hubs)


def dense_hub(code, weight, count, hubs, degree):
    def to_owner(x):
        return lax.all_to_all(
            x.reshape(N_ROW * N_COL, -1), ("row", "col"), split_axis=0, concat_axis=0, tiled=True
        )

    codes, weights, counts = to_owner(code), to_owner(weight), to_owner(count)
    usable = jnp.arange(CAP, dtype=jnp.int32)[None, :] < counts
    weights = jnp.where(usable, weights, jnp.zeros((), BF16)).reshape(-1)
    codes = codes.reshape(-1) - TILES_DEV * TILE * TILE

    def step(turn, sums):
        part = lax.dynamic_slice_in_dim(codes, turn * 512, 512)
        value = lax.dynamic_slice_in_dim(weights, turn * 512, 512)
        left = jnp.where(
            (part >> 9)[:, None] == jnp.arange(HUBS * TILE, dtype=jnp.int32)[None, :],
            value[:, None], jnp.zeros((), BF16),
        )
        right = ((part & 511)[:, None] == jnp.arange(TILE, dtype=jnp.int32)[None, :]).astype(BF16)
        return sums + lax.dot_general(
            left, right, (((0,), (0,)), ((), ())), preferred_element_type=F32
        )

    sums = lax.fori_loop(
        0, codes.shape[0] // 512, step, jnp.zeros((HUBS * TILE, TILE), F32)
    )
    sums = sums.reshape(N_COL, HUBS * TILE // N_COL, TILE)
    sums = jnp.sum(lax.all_to_all(sums, "col", 0, 0, tiled=True), axis=0)
    slab_rows = HUBS * TILE // N_COL
    offset = lax.axis_index("col") * slab_rows
    degrees = to_owner(jnp.broadcast_to(degree, (N_ROW * N_COL, TILE)))
    scaling = jnp.mean(degrees)
    pair = lax.dynamic_index_in_dim(hubs[0], offset // TILE, 0, keepdims=False)
    row_degree = lax.dynamic_index_in_dim(degrees, pair[0], 0, keepdims=False)
    row_degree = lax.dynamic_slice_in_dim(row_degree, lax.rem(offset, TILE), slab_rows)
    col_degree = lax.dynamic_index_in_dim(degrees, pair[1], 0, keepdims=False)
    return jnp.log(
        jnp.maximum(scaling * sums / (row_degree[:, None] * col_degree[None, :]), 1.0)
    )


def in_hbm(x):
    return pltpu.with_memory_space_constraint(x, pltpu.HBM)


def shards(edge_code, edge_weight, edge_count, tile_blocks, hub_blocks, node_degree):
    slots, degrees = exchange(
        in_hbm(edge_code.reshape(32, LANES)), in_hbm(edge_weight), in_hbm(edge_count),
        in_hbm(node_degree.reshape(4, LANES)),
    )
    degrees = degrees.reshape(N_COL * N_ROW, 4, LANES)
    owned, hub, crowded = tiles(
        slots.reshape(-1, LANES), degrees, in_hbm(tile_blocks.transpose(0, 2, 1)), in_hbm(hub_blocks)
    )
    def dense(_):
        hub = dense_hub(edge_code, edge_weight, edge_count, hub_blocks, node_degree)
        return jnp.zeros_like(crowded), hub

    _, hub = lax.while_loop(lambda state: state[0][0, 0] > 0, dense, (crowded, hub))
    return owned, hub


def solution(mesh):
    both = ("row", "col")
    return jax.shard_map(
        shards,
        mesh=mesh,
        in_specs=(
            P(both, None), P(both, None), P(both, None),
            P(both, None, None), P("row", None, None), P(both, None),
        ),
        out_specs=(P(both, None, None), P(both, None)),
        check_vma=False,
    )
```

```python
import jax
import jax.numpy as jnp
from jax import lax
from jax.experimental import pallas as pl
from jax.experimental.pallas import tpu as pltpu
from jax.sharding import PartitionSpec as P

TILE = 512
TILES_DEV = 4
HUBS = 2
CAP = 32
N_ROW = 8
N_COL = 16
LANES = 128
CHUNK = 256
CHUNKS = TILES_DEV * TILE // CHUNK
FULL = 1 << 22
SPAN = 2
HUB_SPAN = 8
MESH = pl.DeviceIdType.MESH
F32 = jnp.float32
BF16 = jnp.bfloat16
NT = (((1,), (1,)), ((), ()))


def iota(shape, dim):
    return lax.broadcasted_iota(jnp.int32, shape, dim)


def one_hot(keys, rows):
    wide = jnp.broadcast_to(keys.astype(BF16), (rows, keys.shape[1]))
    return wide == iota((rows, keys.shape[1]), 0).astype(BF16)


def weighted(mask, values):
    return jnp.where(mask, jnp.broadcast_to(values.astype(BF16), mask.shape), jnp.zeros((), BF16))


def ones_where(mask):
    return jnp.where(mask, jnp.ones((), BF16), jnp.zeros((), BF16))


def two_rows(x, index):
    return jnp.concatenate([x[2 * index : 2 * index + 1], x[2 * index + 1 : 2 * index + 2]], axis=1)


def arrange(slots_ref, fields, hub_fields, marks):
    turned = slots_ref[...].reshape(N_ROW * N_COL, LANES).T
    code = turned[0:32].astype(jnp.int32)
    crowded = jnp.max(code.astype(F32), axis=(0, 1), keepdims=True)
    code = code & (FULL - 1)
    weight = turned[32:64]
    cell = turned[64:96].astype(jnp.int32)
    hub_weight = turned[96:128]
    hub_fields[0] = (((cell >> 8) & 1) * 64 + (cell >> 9)).astype(F32)
    hub_fields[1] = (cell & 255).astype(F32)
    hub_fields[2] = hub_weight
    used = jnp.where(hub_weight > 0.0, iota((32, LANES), 0) + HUB_SPAN, 0).astype(F32)
    used = jnp.max(used, axis=(0, 1), keepdims=True)

    chunk = jnp.where(weight > 0.0, code >> 17, CHUNKS)
    member = jnp.concatenate([ones_where(chunk == q) for q in range(CHUNKS)], axis=0)
    upto = ones_where(jnp.logical_or(
        iota((LANES, 256), 0) <= iota((LANES, 256), 1), iota((LANES, 256), 1) >= LANES
    ))
    inside = jnp.dot(member, upto, preferred_element_type=F32)
    inside, lines = inside[:, :LANES], inside[:, LANES:]
    before = ones_where(iota((256, 256), 1) < iota((256, 256), 0))
    base = jnp.dot(before, lines.astype(BF16), preferred_element_type=F32)
    rank = base + inside - 1.0
    place = jnp.full((32, LANES), -1.0, F32)
    for q in range(CHUNKS):
        place = jnp.where(chunk == q, rank[32 * q : 32 * q + 32], place)
    place = place.astype(jnp.int32)
    for q in range(CHUNKS):
        marks[pl.ds(q, 1), :] = base[32 * q : 32 * q + 1]
    marks[pl.ds(8, 1), :] = base[255:256] + lines[255:256]
    marks[pl.ds(9, 1), :] = jnp.broadcast_to(used, (1, LANES))
    marks[pl.ds(10, 6), :] = jnp.broadcast_to(crowded, (6, LANES))

    high, low = (place >> 7).astype(F32), (place & 127).astype(F32)
    parts = (
        (code & 255).astype(F32),
        (((code >> 8) & 1) + 2 * (code >> 17)).astype(F32),
        ((code >> 9) & 255).astype(F32),
        weight,
    )
    moved = jnp.zeros((LANES, LANES), F32)
    for p in range(16):
        mask = one_hot(two_rows(high, p), 32)
        left = jnp.concatenate([weighted(mask, two_rows(part, p)) for part in parts], axis=0)
        right = ones_where(one_hot(two_rows(low, p), LANES))
        moved += lax.dot_general(left, right, NT, preferred_element_type=F32)
    flags = moved[32:64].astype(jnp.int32)
    column = moved[0:32] + ((flags & 1) * 256).astype(F32)
    fields[:, pl.ds(32, 8), :] = jnp.zeros((4, 8, LANES), F32)
    fields[0, 0:32] = moved[64:96] + ((flags >> 1) * 256).astype(F32)
    fields[1, 0:32] = column
    fields[2, 0:32] = column - 256.0
    fields[3, 0:32] = moved[96:128]


def exchange_kernel(
    code_hbm, weight_hbm, count_hbm, degree_hbm,
    fields, hub_fields, marks, degrees_a, degrees_b,
    code_ref, weight_ref, count_ref, wide, own_part, message, relay, slots_ref,
    in_sem, row_send, row_recv, col_send, col_recv, turn_send, turn_recv, local_sem,
):
    row = lax.axis_index("row")
    col = lax.axis_index("col")
    row_peers = [lax.rem(row + k, N_ROW) for k in range(1, N_ROW)]
    col_peers = [lax.rem(col + k, N_COL) for k in range(1, N_COL)]

    barrier = pltpu.get_barrier_semaphore()
    for peer in col_peers:
        pl.semaphore_signal(barrier, inc=1, device_id=(row, peer), device_id_type=MESH)
    for peer in row_peers:
        pl.semaphore_signal(barrier, inc=1, device_id=(peer, col), device_id_type=MESH)
    mine_a, mine_b = degrees_a.at[col, row], degrees_b.at[row, col]
    inputs = [
        pltpu.make_async_copy(src, dst, in_sem.at[i])
        for i, (src, dst) in enumerate((
            (count_hbm, count_ref), (weight_hbm, weight_ref), (code_hbm, code_ref),
            (degree_hbm.at[0], mine_a), (degree_hbm.at[1], mine_b),
        ))
    ]
    for copy in inputs:
        copy.start()
    for copy in inputs:
        copy.wait()

    lane = iota((32, LANES), 1)
    line = iota((32, LANES), 0)
    counts = jnp.where(lane // 4 == line, jnp.broadcast_to(count_ref[...], (32, LANES)), 0)
    spread = ones_where(iota((LANES, LANES), 0) % 4 == iota((LANES, LANES), 1) // CAP)
    counts = jnp.dot(counts.astype(BF16), spread, preferred_element_type=F32)
    for g in range(32):
        wide[pl.ds(g, 1), :] = weight_ref[:, pl.ds(g * LANES, LANES)].astype(F32)
    weights = jnp.where((lane % CAP).astype(F32) < counts, wide[...], 0.0)
    codes = code_ref[...]

    slab = jnp.where(weights > 0.0, (codes >> 15) - 32, -1)
    member = jnp.concatenate([ones_where(slab == j) for j in range(N_COL)], axis=0)
    upto = ones_where(jnp.logical_or(
        iota((LANES, 256), 0) <= iota((LANES, 256), 1), iota((LANES, 256), 1) >= LANES
    ))
    inside = jnp.dot(member, upto, preferred_element_type=F32)
    near = jnp.logical_and(
        iota((256, 256), 0) // 4 == iota((256, 256), 1) // 4, iota((256, 256), 1) < iota((256, 256), 0)
    )
    near = ones_where(near)
    rank = jnp.full((32, LANES), -1.0, F32)
    for half in range(2):
        part = inside[256 * half : 256 * half + 256]
        base = jnp.dot(near, part[:, LANES:].astype(BF16), preferred_element_type=F32)
        part = base + part[:, :LANES] - 1.0
        for j in range(8):
            rank = jnp.where(slab == 8 * half + j, part[32 * j : 32 * j + 32], rank)
    crowded = (jnp.max(rank, axis=(0, 1), keepdims=True) >= CAP).astype(F32) * FULL

    slab = slab.astype(F32)
    cell_low = (codes & 255).astype(F32)
    cell_high = ((codes >> 8) & 127).astype(F32)
    packed = []
    for r in range(N_ROW):
        part = jnp.zeros((N_COL, LANES), F32)
        for h in range(2):
            p = 2 * r + h
            mask = one_hot(two_rows(rank, p), CAP)
            none = jnp.zeros((CAP, 256), BF16)
            right = jnp.concatenate([
                weighted(mask, two_rows(cell_low, p)), none,
                weighted(mask, two_rows(cell_high, p)), weighted(mask, two_rows(weights, p)),
            ], axis=0)
            left = ones_where(one_hot(two_rows(slab, p), N_COL))
            part += lax.dot_general(left, right, NT, preferred_element_type=F32)
        packed.append(part)
    packed = jnp.concatenate(packed, axis=0)
    lanes = iota((LANES, LANES), 1)
    packed = jnp.where(lanes < 96, packed * 256.0 + pltpu.roll(packed, 64, axis=1), packed)

    flagged = codes.astype(F32) + crowded
    for u in range(4):
        left = pltpu.roll(flagged, (LANES - CAP * u) % LANES, axis=1)
        right = pltpu.roll(weights, (LANES + CAP - CAP * u) % LANES, axis=1)
        own_part[pl.ds(u, 32, stride=4), :] = jnp.where(lane < CAP, left, right)
    lines = jnp.where(lanes < 64, own_part[...], packed)
    for d in range(N_ROW * N_COL):
        message[d // N_COL, d % N_COL] = lines[d : d + 1]

    pl.semaphore_wait(barrier, N_ROW + N_COL - 2)

    def send(src, dst, send_sem, recv_sem, device):
        pltpu.make_async_remote_copy(
            src_ref=src, dst_ref=dst, send_sem=send_sem, recv_sem=recv_sem,
            device_id=device, device_id_type=MESH,
        ).start()

    for peer in row_peers:
        send(message.at[peer], relay.at[:, row], row_send.at[0], row_recv.at[0], (peer, col))
    for peer in row_peers:
        send(mine_a, mine_a, row_send.at[1], row_recv.at[1], (peer, col))
    for peer in col_peers:
        send(mine_b, mine_b, turn_send.at[0], turn_recv.at[0], (row, peer))
    own = pltpu.make_async_copy(message.at[row], relay.at[:, row], local_sem.at[0])
    own.start()
    own.wait()
    row_others, col_others = pl.ds(0, N_ROW - 1), pl.ds(0, N_COL - 1)

    def settle(ref, sem):
        pltpu.make_async_copy(ref, ref, sem).wait()

    settle(relay.at[:, row_others], row_recv.at[0])
    for peer in col_peers:
        send(relay.at[peer, :, 0], slots_ref.at[col], col_send.at[0], col_recv.at[0], (row, peer))
    own = pltpu.make_async_copy(relay.at[col, :, 0], slots_ref.at[col], local_sem.at[1])
    own.start()
    settle(degrees_a.at[0, row_others], row_recv.at[1])
    for peer in col_peers:
        send(degrees_a.at[col], degrees_a.at[col], col_send.at[1], col_recv.at[1], (row, peer))
    settle(degrees_b.at[0, col_others], turn_recv.at[0])
    for peer in row_peers:
        send(degrees_b.at[row], degrees_b.at[row], turn_send.at[1], turn_recv.at[1], (peer, col))
    own.wait()
    settle(slots_ref.at[col_others], col_recv.at[0])

    arrange(slots_ref, fields, hub_fields, marks)

    settle(relay.at[:, row_others], row_send.at[0])
    settle(degrees_a.at[0, row_others], row_send.at[1])
    settle(degrees_b.at[0, col_others], turn_send.at[0])
    settle(slots_ref.at[col_others], col_send.at[0])
    settle(degrees_a.at[col_others], col_send.at[1])
    settle(degrees_b.at[row_others], turn_send.at[1])
    settle(degrees_a.at[col_others], col_recv.at[1])
    settle(degrees_b.at[row_others], turn_recv.at[1])


def exchange(code, weight, count, degree):
    vmem = pl.BlockSpec(memory_space=pltpu.VMEM)
    hbm = pl.BlockSpec(memory_space=pltpu.HBM)
    pair = pltpu.SemaphoreType.DMA((2,))
    return pl.pallas_call(
        exchange_kernel,
        out_shape=(
            jax.ShapeDtypeStruct((4, 40, LANES), F32),
            jax.ShapeDtypeStruct((3, 32, LANES), F32),
            jax.ShapeDtypeStruct((16, LANES), F32),
            jax.ShapeDtypeStruct((N_COL, N_ROW, 2, LANES), F32),
            jax.ShapeDtypeStruct((N_ROW, N_COL, 2, LANES), F32),
        ),
        in_specs=[hbm] * 4,
        out_specs=(vmem,) * 5,
        scratch_shapes=[
            pltpu.VMEM((32, LANES), jnp.int32),
            pltpu.VMEM((1, N_ROW * N_COL * CAP), BF16),
            pltpu.VMEM((1, LANES), jnp.int32),
            pltpu.VMEM((32, LANES), F32),
            pltpu.VMEM((LANES, LANES), F32),
            pltpu.VMEM((N_ROW, N_COL, 1, LANES), F32),
            pltpu.VMEM((N_COL, N_ROW, 1, LANES), F32),
            pltpu.VMEM((N_COL, N_ROW, LANES), F32),
            pltpu.SemaphoreType.DMA((5,)),
            pair, pair, pair, pair, pair, pair, pair,
        ],
        compiler_params=pltpu.CompilerParams(
            collective_id=0, has_side_effects=True, vmem_limit_bytes=16 << 20
        ),
    )(code, weight, count, degree)


def stored(block):
    return lax.rem(block, N_COL) * N_ROW + block // N_COL


def tile_kernel(
    fields, hub_fields, marks, degrees_a, degrees_b, blocks_hbm, hubs_hbm,
    owned_ref, hub_out, crowded_out, blocks_ref, hubs_ref, crowded_ref, total, hub_total, staged, hub_ref, gathered,
    in_sem, out_sem, flag_sem,
):
    col = lax.axis_index("col")
    inputs = (
        pltpu.make_async_copy(blocks_hbm, blocks_ref, in_sem.at[0]),
        pltpu.make_async_copy(hubs_hbm, hubs_ref, in_sem.at[1]),
    )
    for copy in inputs:
        copy.start()

    def mark(k):
        return jnp.max(marks[pl.ds(k, 1), :]).astype(jnp.int32)

    starts = [mark(q) for q in range(CHUNKS + 1)]
    used = mark(9) // HUB_SPAN
    crowded_ref[0, 0] = (mark(10) >= FULL).astype(jnp.int32)
    flag_copy = pltpu.make_async_copy(crowded_ref, crowded_out, flag_sem)
    flag_copy.start()

    def degrees_of(block):
        return jnp.concatenate([degrees_a[stored(block)], degrees_b[block]], axis=0)

    def out_copy(q):
        return pltpu.make_async_copy(
            staged.at[q], owned_ref.at[q // 2, pl.ds(CHUNK * (q % 2), CHUNK)], out_sem.at[q]
        )

    def product(b, q):
        def line(f):
            return jnp.concatenate(
                [fields[f, pl.ds(2 * b + i, 1), :] for i in range(2 * SPAN)], axis=1
            )

        left = weighted(one_hot(line(0) - 256.0 * q, CHUNK), line(3))
        right = jnp.concatenate(
            [ones_where(one_hot(line(1), 256)), ones_where(one_hot(line(2), 256))], axis=0
        )
        return lax.dot_general(left, right, NT, preferred_element_type=F32)

    firsts = [starts[q] >> 8 for q in range(CHUNKS)]

    def add_rest(q):
        def add_blocks(i, _):
            total[q % 2] += product(firsts[q] + SPAN * i, q)
            return 0

        blocks = ((starts[q + 1] + 255) >> 8) - firsts[q]
        lax.fori_loop(1, (blocks + SPAN - 1) // SPAN, add_blocks, 0)

    total[0] = product(firsts[0], 0)
    add_rest(0)

    scaling = jnp.sum(degrees_a[...], axis=0) + jnp.sum(degrees_b[...], axis=0)
    scaling = jnp.sum(scaling) / (N_ROW * N_COL * TILE)
    for copy in inputs:
        copy.wait()
    gathered[...] = jnp.ones_like(gathered)
    for t in range(TILES_DEV):
        gathered[pl.ds(4 * t, 4), :] = degrees_of(blocks_ref[0, 0, t])
    hub = col // 8
    gathered[pl.ds(24, 4), :] = degrees_of(hubs_ref[0, hub, 0])
    hub_row = gathered[pl.ds(24 + lax.rem(col, 8) // 2, 1), :]
    gathered[pl.ds(16, 8), :] = pltpu.roll(
        jnp.broadcast_to(hub_row, (8, LANES)), 64 * lax.rem(col, 2), axis=1
    )
    degree_rows = (scaling / gathered[...]).T

    def hub_product(b):
        def line(f):
            return jnp.concatenate(
                [hub_fields[f, pl.ds(HUB_SPAN * b + i, 1), :] for i in range(HUB_SPAN)], axis=1
            )

        return lax.dot_general(
            weighted(one_hot(line(0), LANES), line(2)), ones_where(one_hot(line(1), 256)),
            NT, preferred_element_type=F32,
        )

    for q in range(CHUNKS):
        if q + 1 < CHUNKS:
            total[(q + 1) % 2] = product(firsts[q + 1], q + 1)
        else:
            hub_total[...] = hub_product(0)
        tile = q // 2
        degree = 1.0 / degrees_of(blocks_ref[0, 1, tile])
        for j in range(2):
            rows = degree_rows[:, 4 * tile + 2 * (q % 2) + j][:, None]
            for n in range(4):
                values = total[q % 2, pl.ds(LANES * j, LANES), pl.ds(LANES * n, LANES)]
                values = values * rows * degree[n : n + 1]
                staged[q, pl.ds(LANES * j, LANES), pl.ds(LANES * n, LANES)] = jnp.log(
                    jnp.maximum(values, 1.0)
                )
        out_copy(q).start()
        if q + 1 < CHUNKS:
            add_rest(q + 1)

    def add_hub(b, _):
        hub_total[...] += hub_product(b)
        return 0

    lax.fori_loop(1, used, add_hub, 0)
    hub_degree = 1.0 / degrees_of(hubs_ref[0, hub, 1])
    for n in range(4):
        values = hub_total[pl.ds(64 * (n // 2), 64), pl.ds(LANES * (n % 2), LANES)]
        values = values * degree_rows[0:64, 16:17] * hub_degree[n : n + 1]
        hub_ref[:, pl.ds(LANES * n, LANES)] = jnp.log(jnp.maximum(values, 1.0))
    hub_copy = pltpu.make_async_copy(hub_ref, hub_out, out_sem.at[CHUNKS])
    hub_copy.start()
    flag_copy.wait()
    hub_copy.wait()
    for q in range(CHUNKS):
        out_copy(q).wait()


def tiles(arranged, blocks, hubs):
    vmem = pl.BlockSpec(memory_space=pltpu.VMEM)
    hbm = pl.BlockSpec(memory_space=pltpu.HBM)
    return pl.pallas_call(
        tile_kernel,
        out_shape=(
            jax.ShapeDtypeStruct((TILES_DEV, TILE, TILE), F32),
            jax.ShapeDtypeStruct((HUBS * TILE // N_COL, TILE), F32),
            jax.ShapeDtypeStruct((1, 1), jnp.int32),
        ),
        in_specs=[vmem] * 5 + [hbm, hbm],
        out_specs=(hbm, hbm, hbm),
        scratch_shapes=[
            pltpu.SMEM((1, 2, TILES_DEV), jnp.int32),
            pltpu.SMEM((1, HUBS, 2), jnp.int32),
            pltpu.SMEM((1, 1), jnp.int32),
            pltpu.VMEM((2, CHUNK, TILE), F32),
            pltpu.VMEM((LANES, 256), F32),
            pltpu.VMEM((CHUNKS, CHUNK, TILE), F32),
            pltpu.VMEM((HUBS * TILE // N_COL, TILE), F32),
            pltpu.VMEM((LANES, LANES), F32),
            pltpu.SemaphoreType.DMA((2,)),
            pltpu.SemaphoreType.DMA((CHUNKS + 1,)),
            pltpu.SemaphoreType.DMA(()),
        ],
        compiler_params=pltpu.CompilerParams(vmem_limit_bytes=32 << 20),
    )(*arranged, blocks, hubs)


def dense_hub(code, weight, count, hubs, degree):
    def to_owner(x):
        return lax.all_to_all(
            x.reshape(N_ROW * N_COL, -1), ("row", "col"), split_axis=0, concat_axis=0, tiled=True
        )

    codes, weights, counts = to_owner(code), to_owner(weight), to_owner(count)
    usable = jnp.arange(CAP, dtype=jnp.int32)[None, :] < counts
    weights = jnp.where(usable, weights, jnp.zeros((), BF16)).reshape(-1)
    codes = codes.reshape(-1) - TILES_DEV * TILE * TILE

    def step(turn, sums):
        part = lax.dynamic_slice_in_dim(codes, turn * 512, 512)
        value = lax.dynamic_slice_in_dim(weights, turn * 512, 512)
        left = jnp.where(
            (part >> 9)[:, None] == jnp.arange(HUBS * TILE, dtype=jnp.int32)[None, :],
            value[:, None], jnp.zeros((), BF16),
        )
        right = ((part & 511)[:, None] == jnp.arange(TILE, dtype=jnp.int32)[None, :]).astype(BF16)
        return sums + lax.dot_general(
            left, right, (((0,), (0,)), ((), ())), preferred_element_type=F32
        )

    sums = lax.fori_loop(
        0, codes.shape[0] // 512, step, jnp.zeros((HUBS * TILE, TILE), F32)
    )
    sums = sums.reshape(N_COL, HUBS * TILE // N_COL, TILE)
    sums = jnp.sum(lax.all_to_all(sums, "col", 0, 0, tiled=True), axis=0)
    slab_rows = HUBS * TILE // N_COL
    offset = lax.axis_index("col") * slab_rows
    degrees = to_owner(jnp.broadcast_to(degree, (N_ROW * N_COL, TILE)))
    scaling = jnp.mean(degrees)
    pair = lax.dynamic_index_in_dim(hubs[0], offset // TILE, 0, keepdims=False)
    row_degree = lax.dynamic_index_in_dim(degrees, pair[0], 0, keepdims=False)
    row_degree = lax.dynamic_slice_in_dim(row_degree, lax.rem(offset, TILE), slab_rows)
    col_degree = lax.dynamic_index_in_dim(degrees, pair[1], 0, keepdims=False)
    return jnp.log(
        jnp.maximum(scaling * sums / (row_degree[:, None] * col_degree[None, :]), 1.0)
    )


def in_hbm(x):
    return pltpu.with_memory_space_constraint(x, pltpu.HBM)


def shards(edge_code, edge_weight, edge_count, tile_blocks, hub_blocks, node_degree):
    fields, hub_fields, marks, degrees_a, degrees_b = exchange(
        in_hbm(edge_code.reshape(32, LANES)), in_hbm(edge_weight), in_hbm(edge_count),
        in_hbm(node_degree.reshape(2, 2, LANES)),
    )
    degrees_a, degrees_b = (x.reshape(-1, 2, LANES) for x in (degrees_a, degrees_b))
    owned, hub, crowded = tiles(
        (fields, hub_fields, marks, degrees_a, degrees_b),
        in_hbm(tile_blocks.transpose(0, 2, 1)), in_hbm(hub_blocks),
    )
    def dense(_):
        hub = dense_hub(edge_code, edge_weight, edge_count, hub_blocks, node_degree)
        return jnp.zeros_like(crowded), hub

    _, hub = lax.while_loop(lambda state: state[0][0, 0] > 0, dense, (crowded, hub))
    return owned, hub


def solution(mesh):
    both = ("row", "col")
    return jax.shard_map(
        shards,
        mesh=mesh,
        in_specs=(
            P(both, None), P(both, None), P(both, None),
            P(both, None, None), P("row", None, None), P(both, None),
        ),
        out_specs=(P(both, None, None), P(both, None)),
        check_vma=False,
    )
```

```python
import jax
import jax.numpy as jnp
from jax import lax
from jax.experimental import pallas as pl
from jax.experimental.pallas import tpu as pltpu
from jax.sharding import PartitionSpec as P

TILE = 512
TILES_DEV = 4
HUBS = 2
CAP = 32
N_ROW = 8
N_COL = 16
LANES = 128
CHUNK = 256
CHUNKS = TILES_DEV * TILE // CHUNK
FULL = 1 << 22
IDS = 11
SPAN = 2
HUB_SPAN = 8
MESH = pl.DeviceIdType.MESH
F32 = jnp.float32
BF16 = jnp.bfloat16
NT = (((1,), (1,)), ((), ()))


def iota(shape, dim):
    return lax.broadcasted_iota(jnp.int32, shape, dim)


def one_hot(keys, rows):
    wide = jnp.broadcast_to(keys.astype(BF16), (rows, keys.shape[1]))
    return wide == iota((rows, keys.shape[1]), 0).astype(BF16)


def weighted(mask, values):
    return jnp.where(mask, jnp.broadcast_to(values.astype(BF16), mask.shape), jnp.zeros((), BF16))


def ones_where(mask):
    return jnp.where(mask, jnp.ones((), BF16), jnp.zeros((), BF16))


def two_rows(x, index):
    return jnp.concatenate([x[2 * index : 2 * index + 1], x[2 * index + 1 : 2 * index + 2]], axis=1)


def arrange(slots_ref, fields, hub_fields, marks):
    turned = slots_ref[...].reshape(N_ROW * N_COL, LANES).T
    code = turned[0:32].astype(jnp.int32)
    crowded = jnp.max(code.astype(F32), axis=(0, 1), keepdims=True)
    code = code & (FULL - 1)
    weight = turned[32:64]
    cell = turned[64:96].astype(jnp.int32)
    hub_weight = turned[96:128]
    hub_fields[0] = (((cell >> 8) & 1) * 64 + (cell >> 9)).astype(F32)
    hub_fields[1] = (cell & 255).astype(F32)
    hub_fields[2] = hub_weight
    used = jnp.where(hub_weight > 0.0, iota((32, LANES), 0) + HUB_SPAN, 0).astype(F32)
    used = jnp.max(used, axis=(0, 1), keepdims=True)

    chunk = jnp.where(weight > 0.0, code >> 17, CHUNKS)
    member = jnp.concatenate([ones_where(chunk == q) for q in range(CHUNKS)], axis=0)
    upto = ones_where(jnp.logical_or(
        iota((LANES, 256), 0) <= iota((LANES, 256), 1), iota((LANES, 256), 1) >= LANES
    ))
    inside = jnp.dot(member, upto, preferred_element_type=F32)
    inside, lines = inside[:, :LANES], inside[:, LANES:]
    before = ones_where(iota((256, 256), 1) < iota((256, 256), 0))
    base = jnp.dot(before, lines.astype(BF16), preferred_element_type=F32)
    rank = base + inside - 1.0
    place = jnp.full((32, LANES), -1.0, F32)
    for q in range(CHUNKS):
        place = jnp.where(chunk == q, rank[32 * q : 32 * q + 32], place)
    place = place.astype(jnp.int32)
    for q in range(CHUNKS):
        marks[pl.ds(q, 1), :] = base[32 * q : 32 * q + 1]
    marks[pl.ds(8, 1), :] = base[255:256] + lines[255:256]
    marks[pl.ds(9, 1), :] = jnp.broadcast_to(used, (1, LANES))
    marks[pl.ds(10, 1), :] = jnp.broadcast_to(crowded, (1, LANES))

    high, low = (place >> 7).astype(F32), (place & 127).astype(F32)
    parts = (
        (code & 255).astype(F32),
        (((code >> 8) & 1) + 2 * (code >> 17)).astype(F32),
        ((code >> 9) & 255).astype(F32),
        weight,
    )
    moved = jnp.zeros((LANES, LANES), F32)
    for p in range(16):
        mask = one_hot(two_rows(high, p), 32)
        left = jnp.concatenate([weighted(mask, two_rows(part, p)) for part in parts], axis=0)
        right = ones_where(one_hot(two_rows(low, p), LANES))
        moved += lax.dot_general(left, right, NT, preferred_element_type=F32)
    flags = moved[32:64].astype(jnp.int32)
    column = moved[0:32] + ((flags & 1) * 256).astype(F32)
    fields[:, pl.ds(32, 8), :] = jnp.zeros((4, 8, LANES), F32)
    fields[0, 0:32] = moved[64:96] + ((flags >> 1) * 256).astype(F32)
    fields[1, 0:32] = column
    fields[2, 0:32] = column - 256.0
    fields[3, 0:32] = moved[96:128]


def exchange_kernel(
    code_hbm, weight_hbm, count_hbm, degree_hbm, blocks_hbm, hubs_hbm,
    fields, hub_fields, marks, degrees_a, degrees_b,
    code_ref, weight_ref, count_ref, blocks_ref, hubs_ref, wide, own_part, message, relay, slots_ref,
    in_sem, row_send, row_recv, col_send, col_recv, turn_send, turn_recv, local_sem,
):
    row = lax.axis_index("row")
    col = lax.axis_index("col")
    row_peers = [lax.rem(row + k, N_ROW) for k in (4, 3, 5, 2, 6, 1, 7)]
    col_peers = [
        lax.rem(col + k, N_COL) for k in (10, 6, 9, 11, 5, 7, 8, 2, 14, 13, 3, 12, 4, 1, 15)
    ]

    mine_a, mine_b = degrees_a.at[col, row], degrees_b.at[row, col]
    inputs = [
        pltpu.make_async_copy(src, dst, in_sem.at[i])
        for i, (src, dst) in enumerate((
            (count_hbm, count_ref), (weight_hbm, weight_ref), (code_hbm, code_ref),
            (degree_hbm.at[0], mine_a), (degree_hbm.at[1], mine_b),
            (blocks_hbm, blocks_ref), (hubs_hbm, hubs_ref),
        ))
    ]
    for copy in inputs:
        copy.start()
    barrier = pltpu.get_barrier_semaphore()
    for peer in col_peers:
        pl.semaphore_signal(barrier, inc=1, device_id=(row, peer), device_id_type=MESH)
    for peer in row_peers:
        pl.semaphore_signal(barrier, inc=1, device_id=(peer, col), device_id_type=MESH)
    for copy in inputs:
        copy.wait()

    lane = iota((32, LANES), 1)
    line = iota((32, LANES), 0)
    counts = jnp.where(lane // 4 == line, jnp.broadcast_to(count_ref[...], (32, LANES)), 0)
    spread = ones_where(iota((LANES, LANES), 0) % 4 == iota((LANES, LANES), 1) // CAP)
    counts = jnp.dot(counts.astype(BF16), spread, preferred_element_type=F32)
    for g in range(32):
        wide[pl.ds(g, 1), :] = weight_ref[:, pl.ds(g * LANES, LANES)].astype(F32)
    weights = jnp.where((lane % CAP).astype(F32) < counts, wide[...], 0.0)
    codes = code_ref[...]

    slab = jnp.where(weights > 0.0, (codes >> 15) - 32, -1)
    member = jnp.concatenate([ones_where(slab == j) for j in range(N_COL)], axis=0)
    upto = ones_where(jnp.logical_or(
        iota((LANES, 256), 0) <= iota((LANES, 256), 1), iota((LANES, 256), 1) >= LANES
    ))
    inside = jnp.dot(member, upto, preferred_element_type=F32)
    near = jnp.logical_and(
        iota((256, 256), 0) // 4 == iota((256, 256), 1) // 4, iota((256, 256), 1) < iota((256, 256), 0)
    )
    near = ones_where(near)
    rank = jnp.full((32, LANES), -1.0, F32)
    for half in range(2):
        part = inside[256 * half : 256 * half + 256]
        base = jnp.dot(near, part[:, LANES:].astype(BF16), preferred_element_type=F32)
        part = base + part[:, :LANES] - 1.0
        for j in range(8):
            rank = jnp.where(slab == 8 * half + j, part[32 * j : 32 * j + 32], rank)
    crowded = (jnp.max(rank, axis=(0, 1), keepdims=True) >= CAP).astype(F32) * FULL

    slab = slab.astype(F32)
    cell_low = (codes & 255).astype(F32)
    cell_high = ((codes >> 8) & 127).astype(F32)
    packed = []
    for r in range(N_ROW):
        part = jnp.zeros((N_COL, LANES), F32)
        for h in range(2):
            p = 2 * r + h
            mask = one_hot(two_rows(rank, p), CAP)
            none = jnp.zeros((CAP, 256), BF16)
            right = jnp.concatenate([
                weighted(mask, two_rows(cell_low, p)), none,
                weighted(mask, two_rows(cell_high, p)), weighted(mask, two_rows(weights, p)),
            ], axis=0)
            left = ones_where(one_hot(two_rows(slab, p), N_COL))
            part += lax.dot_general(left, right, NT, preferred_element_type=F32)
        packed.append(part)
    packed = jnp.concatenate(packed, axis=0)
    lanes = iota((LANES, LANES), 1)
    packed = jnp.where(lanes < 96, packed * 256.0 + pltpu.roll(packed, 64, axis=1), packed)

    flagged = codes.astype(F32) + crowded
    for u in range(4):
        left = pltpu.roll(flagged, (LANES - CAP * u) % LANES, axis=1)
        right = pltpu.roll(weights, (LANES + CAP - CAP * u) % LANES, axis=1)
        own_part[pl.ds(u, 32, stride=4), :] = jnp.where(lane < CAP, left, right)
    lines = jnp.where(lanes < 64, own_part[...], packed)
    for d in range(N_ROW * N_COL):
        message[d // N_COL, d % N_COL] = lines[d : d + 1]

    pl.semaphore_wait(barrier, N_ROW + N_COL - 2)

    def send(src, dst, send_sem, recv_sem, device):
        pltpu.make_async_remote_copy(
            src_ref=src, dst_ref=dst, send_sem=send_sem, recv_sem=recv_sem,
            device_id=device, device_id_type=MESH,
        ).start()

    for peer in row_peers:
        send(message.at[peer], relay.at[:, row], row_send.at[0], row_recv.at[0], (peer, col))
    for peer in row_peers:
        send(mine_a, mine_a, row_send.at[1], row_recv.at[1], (peer, col))
    for peer in col_peers:
        send(mine_b, mine_b, turn_send.at[0], turn_recv.at[0], (row, peer))
    own = pltpu.make_async_copy(message.at[row], relay.at[:, row], local_sem.at[0])
    own.start()
    own.wait()
    row_others, col_others = pl.ds(0, N_ROW - 1), pl.ds(0, N_COL - 1)

    def settle(ref, sem):
        pltpu.make_async_copy(ref, ref, sem).wait()

    settle(relay.at[:, row_others], row_recv.at[0])
    for peer in col_peers:
        send(relay.at[peer, :, 0], slots_ref.at[col], col_send.at[0], col_recv.at[0], (row, peer))
    own = pltpu.make_async_copy(relay.at[col, :, 0], slots_ref.at[col], local_sem.at[1])
    own.start()
    settle(degrees_a.at[0, row_others], row_recv.at[1])
    for peer in col_peers:
        send(degrees_a.at[col], degrees_a.at[col], col_send.at[1], col_recv.at[1], (row, peer))
    settle(degrees_b.at[0, col_others], turn_recv.at[0])
    for peer in row_peers:
        send(degrees_b.at[row], degrees_b.at[row], turn_send.at[1], turn_recv.at[1], (peer, col))
    own.wait()
    settle(slots_ref.at[col_others], col_recv.at[0])

    arrange(slots_ref, fields, hub_fields, marks)
    ids = [blocks_ref[0, side, t] for side in range(2) for t in range(TILES_DEV)]
    ids += [hubs_ref[0, col // 8, side] for side in range(2)]
    for k, block in enumerate(ids):
        marks[pl.ds(IDS + k, 1), :] = jnp.full((1, LANES), block, jnp.int32).astype(F32)

    settle(relay.at[:, row_others], row_send.at[0])
    settle(degrees_a.at[0, row_others], row_send.at[1])
    settle(degrees_b.at[0, col_others], turn_send.at[0])
    settle(slots_ref.at[col_others], col_send.at[0])
    settle(degrees_a.at[col_others], col_send.at[1])
    settle(degrees_b.at[row_others], turn_send.at[1])
    settle(degrees_a.at[col_others], col_recv.at[1])
    settle(degrees_b.at[row_others], turn_recv.at[1])


def exchange(code, weight, count, degree, blocks, hubs):
    vmem = pl.BlockSpec(memory_space=pltpu.VMEM)
    hbm = pl.BlockSpec(memory_space=pltpu.HBM)
    pair = pltpu.SemaphoreType.DMA((2,))
    return pl.pallas_call(
        exchange_kernel,
        out_shape=(
            jax.ShapeDtypeStruct((4, 40, LANES), F32),
            jax.ShapeDtypeStruct((3, 32, LANES), F32),
            jax.ShapeDtypeStruct((24, LANES), F32),
            jax.ShapeDtypeStruct((N_COL, N_ROW, 2, LANES), F32),
            jax.ShapeDtypeStruct((N_ROW, N_COL, 2, LANES), F32),
        ),
        in_specs=[hbm] * 6,
        out_specs=(vmem,) * 5,
        scratch_shapes=[
            pltpu.VMEM((32, LANES), jnp.int32),
            pltpu.VMEM((1, N_ROW * N_COL * CAP), BF16),
            pltpu.VMEM((1, LANES), jnp.int32),
            pltpu.SMEM((1, 2, TILES_DEV), jnp.int32),
            pltpu.SMEM((1, HUBS, 2), jnp.int32),
            pltpu.VMEM((32, LANES), F32),
            pltpu.VMEM((LANES, LANES), F32),
            pltpu.VMEM((N_ROW, N_COL, 1, LANES), F32),
            pltpu.VMEM((N_COL, N_ROW, 1, LANES), F32),
            pltpu.VMEM((N_COL, N_ROW, LANES), F32),
            pltpu.SemaphoreType.DMA((7,)),
            pair, pair, pair, pair, pair, pair, pair,
        ],
        compiler_params=pltpu.CompilerParams(
            collective_id=0, has_side_effects=True, vmem_limit_bytes=16 << 20
        ),
    )(code, weight, count, degree, blocks, hubs)


def stored(block):
    return lax.rem(block, N_COL) * N_ROW + block // N_COL


def tile_kernel(
    fields, hub_fields, marks, degrees_a, degrees_b,
    owned_ref, hub_out, crowded_out, crowded_ref, total, hub_total, staged, hub_ref, gathered,
    out_sem, flag_sem,
):
    col = lax.axis_index("col")

    def mark(k):
        return jnp.max(marks[pl.ds(k, 1), :]).astype(jnp.int32)

    starts = [mark(q) for q in range(CHUNKS + 1)]
    used = mark(9) // HUB_SPAN
    crowded_ref[0, 0] = (mark(10) >= FULL).astype(jnp.int32)
    flag_copy = pltpu.make_async_copy(crowded_ref, crowded_out, flag_sem)
    flag_copy.start()

    row_blocks = [mark(IDS + t) for t in range(TILES_DEV)]
    col_blocks = [mark(IDS + TILES_DEV + t) for t in range(TILES_DEV)]
    hub_row_block, hub_col_block = mark(IDS + 2 * TILES_DEV), mark(IDS + 2 * TILES_DEV + 1)

    def degrees_of(block):
        return jnp.concatenate([degrees_a[stored(block)], degrees_b[block]], axis=0)

    def out_copy(q):
        return pltpu.make_async_copy(
            staged.at[q], owned_ref.at[q // 2, pl.ds(CHUNK * (q % 2), CHUNK)], out_sem.at[q]
        )

    def product(b, q):
        def line(f):
            return jnp.concatenate(
                [fields[f, pl.ds(2 * b + i, 1), :] for i in range(2 * SPAN)], axis=1
            )

        left = weighted(one_hot(line(0) - 256.0 * q, CHUNK), line(3))
        right = jnp.concatenate(
            [ones_where(one_hot(line(1), 256)), ones_where(one_hot(line(2), 256))], axis=0
        )
        return lax.dot_general(left, right, NT, preferred_element_type=F32)

    firsts = [starts[q] >> 8 for q in range(CHUNKS)]

    def add_rest(q):
        def add_blocks(i, _):
            total[q % 2] += product(firsts[q] + SPAN * i, q)
            return 0

        blocks = ((starts[q + 1] + 255) >> 8) - firsts[q]
        lax.fori_loop(1, (blocks + SPAN - 1) // SPAN, add_blocks, 0)

    total[0] = product(firsts[0], 0)
    add_rest(0)

    scaling = jnp.sum(degrees_a[...], axis=0) + jnp.sum(degrees_b[...], axis=0)
    scaling = jnp.sum(scaling) / (N_ROW * N_COL * TILE)
    gathered[...] = jnp.ones_like(gathered)
    for t in range(TILES_DEV):
        gathered[pl.ds(4 * t, 4), :] = degrees_of(row_blocks[t])
    gathered[pl.ds(24, 4), :] = degrees_of(hub_row_block)
    hub_row = gathered[pl.ds(24 + lax.rem(col, 8) // 2, 1), :]
    gathered[pl.ds(16, 8), :] = pltpu.roll(
        jnp.broadcast_to(hub_row, (8, LANES)), 64 * lax.rem(col, 2), axis=1
    )
    degree_rows = (scaling / gathered[...]).T

    def hub_product(b):
        def line(f):
            return jnp.concatenate(
                [hub_fields[f, pl.ds(HUB_SPAN * b + i, 1), :] for i in range(HUB_SPAN)], axis=1
            )

        return lax.dot_general(
            weighted(one_hot(line(0), LANES), line(2)), ones_where(one_hot(line(1), 256)),
            NT, preferred_element_type=F32,
        )

    for q in range(CHUNKS):
        if q + 1 < CHUNKS:
            total[(q + 1) % 2] = product(firsts[q + 1], q + 1)
        else:
            hub_total[...] = hub_product(0)
        tile = q // 2
        degree = 1.0 / degrees_of(col_blocks[tile])
        for j in range(2):
            rows = degree_rows[:, 4 * tile + 2 * (q % 2) + j][:, None]
            for n in range(4):
                values = total[q % 2, pl.ds(LANES * j, LANES), pl.ds(LANES * n, LANES)]
                values = values * rows * degree[n : n + 1]
                staged[q, pl.ds(LANES * j, LANES), pl.ds(LANES * n, LANES)] = jnp.log(
                    jnp.maximum(values, 1.0)
                )
        out_copy(q).start()
        if q + 1 < CHUNKS:
            add_rest(q + 1)

    def add_hub(b, _):
        hub_total[...] += hub_product(b)
        return 0

    lax.fori_loop(1, used, add_hub, 0)
    hub_degree = 1.0 / degrees_of(hub_col_block)
    for n in range(4):
        values = hub_total[pl.ds(64 * (n // 2), 64), pl.ds(LANES * (n % 2), LANES)]
        values = values * degree_rows[0:64, 16:17] * hub_degree[n : n + 1]
        hub_ref[:, pl.ds(LANES * n, LANES)] = jnp.log(jnp.maximum(values, 1.0))
    hub_copy = pltpu.make_async_copy(hub_ref, hub_out, out_sem.at[CHUNKS])
    hub_copy.start()
    flag_copy.wait()
    hub_copy.wait()
    for q in range(CHUNKS):
        out_copy(q).wait()


def tiles(*arranged):
    vmem = pl.BlockSpec(memory_space=pltpu.VMEM)
    hbm = pl.BlockSpec(memory_space=pltpu.HBM)
    return pl.pallas_call(
        tile_kernel,
        out_shape=(
            jax.ShapeDtypeStruct((TILES_DEV, TILE, TILE), F32),
            jax.ShapeDtypeStruct((HUBS * TILE // N_COL, TILE), F32),
            jax.ShapeDtypeStruct((1, 1), jnp.int32),
        ),
        in_specs=[vmem] * 5,
        out_specs=(hbm, hbm, hbm),
        scratch_shapes=[
            pltpu.SMEM((1, 1), jnp.int32),
            pltpu.VMEM((2, CHUNK, TILE), F32),
            pltpu.VMEM((LANES, 256), F32),
            pltpu.VMEM((CHUNKS, CHUNK, TILE), F32),
            pltpu.VMEM((HUBS * TILE // N_COL, TILE), F32),
            pltpu.VMEM((LANES, LANES), F32),
            pltpu.SemaphoreType.DMA((CHUNKS + 1,)),
            pltpu.SemaphoreType.DMA(()),
        ],
        compiler_params=pltpu.CompilerParams(vmem_limit_bytes=32 << 20),
    )(*arranged)


def dense_hub(code, weight, count, hubs, degree):
    def to_owner(x):
        return lax.all_to_all(
            x.reshape(N_ROW * N_COL, -1), ("row", "col"), split_axis=0, concat_axis=0, tiled=True
        )

    codes, weights, counts = to_owner(code), to_owner(weight), to_owner(count)
    usable = jnp.arange(CAP, dtype=jnp.int32)[None, :] < counts
    weights = jnp.where(usable, weights, jnp.zeros((), BF16)).reshape(-1)
    codes = codes.reshape(-1) - TILES_DEV * TILE * TILE

    def step(turn, sums):
        part = lax.dynamic_slice_in_dim(codes, turn * 512, 512)
        value = lax.dynamic_slice_in_dim(weights, turn * 512, 512)
        left = jnp.where(
            (part >> 9)[:, None] == jnp.arange(HUBS * TILE, dtype=jnp.int32)[None, :],
            value[:, None], jnp.zeros((), BF16),
        )
        right = ((part & 511)[:, None] == jnp.arange(TILE, dtype=jnp.int32)[None, :]).astype(BF16)
        return sums + lax.dot_general(
            left, right, (((0,), (0,)), ((), ())), preferred_element_type=F32
        )

    sums = lax.fori_loop(
        0, codes.shape[0] // 512, step, jnp.zeros((HUBS * TILE, TILE), F32)
    )
    sums = sums.reshape(N_COL, HUBS * TILE // N_COL, TILE)
    sums = jnp.sum(lax.all_to_all(sums, "col", 0, 0, tiled=True), axis=0)
    slab_rows = HUBS * TILE // N_COL
    offset = lax.axis_index("col") * slab_rows
    degrees = to_owner(jnp.broadcast_to(degree, (N_ROW * N_COL, TILE)))
    scaling = jnp.mean(degrees)
    pair = lax.dynamic_index_in_dim(hubs[0], offset // TILE, 0, keepdims=False)
    row_degree = lax.dynamic_index_in_dim(degrees, pair[0], 0, keepdims=False)
    row_degree = lax.dynamic_slice_in_dim(row_degree, lax.rem(offset, TILE), slab_rows)
    col_degree = lax.dynamic_index_in_dim(degrees, pair[1], 0, keepdims=False)
    return jnp.log(
        jnp.maximum(scaling * sums / (row_degree[:, None] * col_degree[None, :]), 1.0)
    )


def in_hbm(x):
    return pltpu.with_memory_space_constraint(x, pltpu.HBM)


def shards(edge_code, edge_weight, edge_count, tile_blocks, hub_blocks, node_degree):
    fields, hub_fields, marks, degrees_a, degrees_b = exchange(
        in_hbm(edge_code.reshape(32, LANES)), in_hbm(edge_weight), in_hbm(edge_count),
        in_hbm(node_degree.reshape(2, 2, LANES)), in_hbm(tile_blocks.transpose(0, 2, 1)),
        in_hbm(hub_blocks),
    )
    degrees_a, degrees_b = (x.reshape(-1, 2, LANES) for x in (degrees_a, degrees_b))
    owned, hub, crowded = tiles(fields, hub_fields, marks, degrees_a, degrees_b)
    def dense(_):
        hub = dense_hub(edge_code, edge_weight, edge_count, hub_blocks, node_degree)
        return jnp.zeros_like(crowded), hub

    _, hub = lax.while_loop(lambda state: state[0][0, 0] > 0, dense, (crowded, hub))
    return owned, hub


def solution(mesh):
    both = ("row", "col")
    return jax.shard_map(
        shards,
        mesh=mesh,
        in_specs=(
            P(both, None), P(both, None), P(both, None),
            P(both, None, None), P("row", None, None), P(both, None),
        ),
        out_specs=(P(both, None, None), P(both, None)),
        check_vma=False,
    )
```

```python
import jax
import jax.numpy as jnp
from jax import lax
from jax.experimental import pallas as pl
from jax.experimental.pallas import tpu as pltpu
from jax.sharding import PartitionSpec as P

TILE = 512
TILES_DEV = 4
HUBS = 2
CAP = 32
N_ROW = 8
N_COL = 16
LANES = 128
CHUNK = 256
CHUNKS = TILES_DEV * TILE // CHUNK
FULL = 1 << 22
IDS = 11
SPAN = 2
HUB_SPAN = 8
MESH = pl.DeviceIdType.MESH
F32 = jnp.float32
BF16 = jnp.bfloat16
NT = (((1,), (1,)), ((), ()))


def iota(shape, dim):
    return lax.broadcasted_iota(jnp.int32, shape, dim)


def one_hot(keys, rows):
    wide = jnp.broadcast_to(keys.astype(BF16), (rows, keys.shape[1]))
    return wide == iota((rows, keys.shape[1]), 0).astype(BF16)


def weighted(mask, values):
    return jnp.where(mask, jnp.broadcast_to(values.astype(BF16), mask.shape), jnp.zeros((), BF16))


def ones_where(mask):
    return jnp.where(mask, jnp.ones((), BF16), jnp.zeros((), BF16))


def two_rows(x, index):
    return jnp.concatenate([x[2 * index : 2 * index + 1], x[2 * index + 1 : 2 * index + 2]], axis=1)


def arrange(slots_ref, fields, hub_fields, marks):
    turned = slots_ref[...].reshape(N_ROW * N_COL, LANES).T
    code = turned[0:32].astype(jnp.int32)
    crowded = jnp.max(code.astype(F32), axis=(0, 1), keepdims=True)
    code = code & (FULL - 1)
    weight = turned[32:64]
    cell = turned[64:96].astype(jnp.int32)
    hub_weight = turned[96:128]
    hub_fields[0] = (((cell >> 8) & 1) * 64 + (cell >> 9)).astype(F32)
    hub_fields[1] = (cell & 255).astype(F32)
    hub_fields[2] = hub_weight
    used = jnp.where(hub_weight > 0.0, iota((32, LANES), 0) + HUB_SPAN, 0).astype(F32)
    used = jnp.max(used, axis=(0, 1), keepdims=True)

    chunk = jnp.where(weight > 0.0, code >> 17, CHUNKS)
    member = jnp.concatenate([ones_where(chunk == q) for q in range(CHUNKS)], axis=0)
    upto = ones_where(jnp.logical_or(
        iota((LANES, 256), 0) <= iota((LANES, 256), 1), iota((LANES, 256), 1) >= LANES
    ))
    inside = jnp.dot(member, upto, preferred_element_type=F32)
    inside, lines = inside[:, :LANES], inside[:, LANES:]
    before = ones_where(iota((256, 256), 1) < iota((256, 256), 0))
    base = jnp.dot(before, lines.astype(BF16), preferred_element_type=F32)
    rank = base + inside - 1.0
    place = jnp.full((32, LANES), -1.0, F32)
    for q in range(CHUNKS):
        place = jnp.where(chunk == q, rank[32 * q : 32 * q + 32], place)
    place = place.astype(jnp.int32)
    for q in range(CHUNKS):
        marks[pl.ds(q, 1), :] = base[32 * q : 32 * q + 1]
    marks[pl.ds(8, 1), :] = base[255:256] + lines[255:256]
    marks[pl.ds(9, 1), :] = jnp.broadcast_to(used, (1, LANES))
    marks[pl.ds(10, 1), :] = jnp.broadcast_to(crowded, (1, LANES))

    high, low = (place >> 7).astype(F32), (place & 127).astype(F32)
    parts = (
        (code & 255).astype(F32),
        (((code >> 8) & 1) + 2 * (code >> 17)).astype(F32),
        ((code >> 9) & 255).astype(F32),
        weight,
    )
    moved = jnp.zeros((LANES, LANES), F32)
    for p in range(16):
        mask = one_hot(two_rows(high, p), 32)
        left = jnp.concatenate([weighted(mask, two_rows(part, p)) for part in parts], axis=0)
        right = ones_where(one_hot(two_rows(low, p), LANES))
        moved += lax.dot_general(left, right, NT, preferred_element_type=F32)
    flags = moved[32:64].astype(jnp.int32)
    column = moved[0:32] + ((flags & 1) * 256).astype(F32)
    fields[:, pl.ds(32, 8), :] = jnp.zeros((4, 8, LANES), F32)
    fields[0, 0:32] = moved[64:96] + ((flags >> 1) * 256).astype(F32)
    fields[1, 0:32] = column
    fields[2, 0:32] = column - 256.0
    fields[3, 0:32] = moved[96:128]


def exchange_kernel(
    code_hbm, weight_hbm, count_hbm, degree_hbm, blocks_hbm, hubs_hbm,
    fields, hub_fields, marks, degrees_a, degrees_b,
    code_ref, weight_ref, count_ref, blocks_ref, hubs_ref, wide, own_part, message, relay, slots_ref,
    in_sem, row_send, row_recv, col_send, col_recv, turn_send, turn_recv, local_sem,
):
    row = lax.axis_index("row")
    col = lax.axis_index("col")
    row_peers = [lax.rem(row + k, N_ROW) for k in (4, 3, 5, 2, 6, 1, 7)]
    col_peers = [
        lax.rem(col + k, N_COL) for k in (10, 6, 9, 11, 5, 7, 8, 2, 14, 13, 3, 12, 4, 1, 15)
    ]

    mine_a, mine_b = degrees_a.at[col, row], degrees_b.at[row, col]
    inputs = [
        pltpu.make_async_copy(src, dst, in_sem.at[i])
        for i, (src, dst) in enumerate((
            (count_hbm, count_ref), (weight_hbm, weight_ref), (code_hbm, code_ref),
            (degree_hbm.at[0], mine_a), (degree_hbm.at[1], mine_b),
            (blocks_hbm, blocks_ref), (hubs_hbm, hubs_ref),
        ))
    ]
    for copy in inputs:
        copy.start()
    barrier = pltpu.get_barrier_semaphore()
    for peer in col_peers:
        pl.semaphore_signal(barrier, inc=1, device_id=(row, peer), device_id_type=MESH)
    for peer in row_peers:
        pl.semaphore_signal(barrier, inc=1, device_id=(peer, col), device_id_type=MESH)
    for copy in inputs:
        copy.wait()

    lane = iota((32, LANES), 1)
    line = iota((32, LANES), 0)
    counts = jnp.where(lane // 4 == line, jnp.broadcast_to(count_ref[...], (32, LANES)), 0)
    spread = ones_where(iota((LANES, LANES), 0) % 4 == iota((LANES, LANES), 1) // CAP)
    counts = jnp.dot(counts.astype(BF16), spread, preferred_element_type=F32)
    for g in range(32):
        wide[pl.ds(g, 1), :] = weight_ref[:, pl.ds(g * LANES, LANES)].astype(F32)
    weights = jnp.where((lane % CAP).astype(F32) < counts, wide[...], 0.0)
    codes = code_ref[...]

    slab = jnp.where(weights > 0.0, (codes >> 15) - 32, -1)
    member = jnp.concatenate([ones_where(slab == j) for j in range(N_COL)], axis=0)
    upto = ones_where(jnp.logical_or(
        iota((LANES, 256), 0) <= iota((LANES, 256), 1), iota((LANES, 256), 1) >= LANES
    ))
    inside = jnp.dot(member, upto, preferred_element_type=F32)
    near = jnp.logical_and(
        iota((256, 256), 0) // 4 == iota((256, 256), 1) // 4, iota((256, 256), 1) < iota((256, 256), 0)
    )
    near = ones_where(near)
    rank = jnp.full((32, LANES), -1.0, F32)
    for half in range(2):
        part = inside[256 * half : 256 * half + 256]
        base = jnp.dot(near, part[:, LANES:].astype(BF16), preferred_element_type=F32)
        part = base + part[:, :LANES] - 1.0
        for j in range(8):
            rank = jnp.where(slab == 8 * half + j, part[32 * j : 32 * j + 32], rank)
    crowded = (jnp.max(rank, axis=(0, 1), keepdims=True) >= CAP).astype(F32) * FULL

    slab = slab.astype(F32)
    cell_low = (codes & 255).astype(F32)
    cell_high = ((codes >> 8) & 127).astype(F32)
    packed = []
    for r in range(N_ROW):
        part = jnp.zeros((N_COL, LANES), F32)
        for h in range(2):
            p = 2 * r + h
            mask = one_hot(two_rows(rank, p), CAP)
            none = jnp.zeros((CAP, 256), BF16)
            right = jnp.concatenate([
                weighted(mask, two_rows(cell_low, p)), none,
                weighted(mask, two_rows(cell_high, p)), weighted(mask, two_rows(weights, p)),
            ], axis=0)
            left = ones_where(one_hot(two_rows(slab, p), N_COL))
            part += lax.dot_general(left, right, NT, preferred_element_type=F32)
        packed.append(part)
    packed = jnp.concatenate(packed, axis=0)
    lanes = iota((LANES, LANES), 1)
    packed = jnp.where(lanes < 96, packed * 256.0 + pltpu.roll(packed, 64, axis=1), packed)

    flagged = codes.astype(F32) + crowded
    for u in range(4):
        left = pltpu.roll(flagged, (LANES - CAP * u) % LANES, axis=1)
        right = pltpu.roll(weights, (LANES + CAP - CAP * u) % LANES, axis=1)
        own_part[pl.ds(u, 32, stride=4), :] = jnp.where(lane < CAP, left, right)
    lines = jnp.where(lanes < 64, own_part[...], packed)
    for d in range(N_ROW * N_COL):
        message[d // N_COL, d % N_COL] = lines[d : d + 1]

    pl.semaphore_wait(barrier, N_ROW + N_COL - 2)

    def send(src, dst, send_sem, recv_sem, device):
        pltpu.make_async_remote_copy(
            src_ref=src, dst_ref=dst, send_sem=send_sem, recv_sem=recv_sem,
            device_id=device, device_id_type=MESH,
        ).start()

    for peer in row_peers:
        send(message.at[peer], relay.at[:, row], row_send.at[0], row_recv.at[0], (peer, col))
    for peer in row_peers:
        send(mine_a, mine_a, row_send.at[1], row_recv.at[1], (peer, col))
    for peer in col_peers:
        send(mine_b, mine_b, turn_send.at[0], turn_recv.at[0], (row, peer))
    own = pltpu.make_async_copy(message.at[row], relay.at[:, row], local_sem.at[0])
    own.start()
    own.wait()
    row_others, col_others = pl.ds(0, N_ROW - 1), pl.ds(0, N_COL - 1)

    def settle(ref, sem):
        pltpu.make_async_copy(ref, ref, sem).wait()

    settle(relay.at[:, row_others], row_recv.at[0])
    for peer in col_peers:
        send(relay.at[peer, :, 0], slots_ref.at[col], col_send.at[0], col_recv.at[0], (row, peer))
    own = pltpu.make_async_copy(relay.at[col, :, 0], slots_ref.at[col], local_sem.at[1])
    own.start()
    settle(degrees_a.at[0, row_others], row_recv.at[1])
    for peer in col_peers:
        send(degrees_a.at[col], degrees_a.at[col], col_send.at[1], col_recv.at[1], (row, peer))
    settle(degrees_b.at[0, col_others], turn_recv.at[0])
    for peer in row_peers:
        send(degrees_b.at[row], degrees_b.at[row], turn_send.at[1], turn_recv.at[1], (peer, col))
    own.wait()
    settle(slots_ref.at[col_others], col_recv.at[0])

    arrange(slots_ref, fields, hub_fields, marks)
    ids = [blocks_ref[0, side, t] for side in range(2) for t in range(TILES_DEV)]
    ids += [hubs_ref[0, col // 8, side] for side in range(2)]
    for k, block in enumerate(ids):
        marks[pl.ds(IDS + k, 1), :] = jnp.full((1, LANES), block, jnp.int32).astype(F32)

    settle(relay.at[:, row_others], row_send.at[0])
    settle(degrees_a.at[0, row_others], row_send.at[1])
    settle(degrees_b.at[0, col_others], turn_send.at[0])
    settle(slots_ref.at[col_others], col_send.at[0])
    settle(degrees_a.at[col_others], col_send.at[1])
    settle(degrees_b.at[row_others], turn_send.at[1])
    settle(degrees_a.at[col_others], col_recv.at[1])
    settle(degrees_b.at[row_others], turn_recv.at[1])


def exchange(code, weight, count, degree, blocks, hubs):
    vmem = pl.BlockSpec(memory_space=pltpu.VMEM)
    hbm = pl.BlockSpec(memory_space=pltpu.HBM)
    pair = pltpu.SemaphoreType.DMA((2,))
    return pl.pallas_call(
        exchange_kernel,
        out_shape=(
            jax.ShapeDtypeStruct((4, 40, LANES), F32),
            jax.ShapeDtypeStruct((3, 32, LANES), F32),
            jax.ShapeDtypeStruct((24, LANES), F32),
            jax.ShapeDtypeStruct((N_COL, N_ROW, 2, LANES), F32),
            jax.ShapeDtypeStruct((N_ROW, N_COL, 2, LANES), F32),
        ),
        in_specs=[hbm] * 6,
        out_specs=(vmem,) * 5,
        scratch_shapes=[
            pltpu.VMEM((32, LANES), jnp.int32),
            pltpu.VMEM((1, N_ROW * N_COL * CAP), BF16),
            pltpu.VMEM((1, LANES), jnp.int32),
            pltpu.SMEM((1, 2, TILES_DEV), jnp.int32),
            pltpu.SMEM((1, HUBS, 2), jnp.int32),
            pltpu.VMEM((32, LANES), F32),
            pltpu.VMEM((LANES, LANES), F32),
            pltpu.VMEM((N_ROW, N_COL, 1, LANES), F32),
            pltpu.VMEM((N_COL, N_ROW, 1, LANES), F32),
            pltpu.VMEM((N_COL, N_ROW, LANES), F32),
            pltpu.SemaphoreType.DMA((7,)),
            pair, pair, pair, pair, pair, pair, pair,
        ],
        compiler_params=pltpu.CompilerParams(
            collective_id=0, has_side_effects=True, vmem_limit_bytes=16 << 20
        ),
    )(code, weight, count, degree, blocks, hubs)


def stored(block):
    return lax.rem(block, N_COL) * N_ROW + block // N_COL


def tile_kernel(
    fields, hub_fields, marks, degrees_a, degrees_b,
    owned_ref, hub_out, crowded_out, crowded_ref, total, hub_total, staged, hub_ref, gathered,
    out_sem, flag_sem,
):
    col = lax.axis_index("col")

    def mark(k):
        return jnp.max(marks[pl.ds(k, 1), :]).astype(jnp.int32)

    starts = [0] + [mark(q) for q in range(1, CHUNKS + 1)]
    used = mark(9) // HUB_SPAN
    crowded_ref[0, 0] = (mark(10) >= FULL).astype(jnp.int32)
    flag_copy = pltpu.make_async_copy(crowded_ref, crowded_out, flag_sem)
    flag_copy.start()

    row_blocks = [mark(IDS + t) for t in range(TILES_DEV)]
    col_blocks = [mark(IDS + TILES_DEV + t) for t in range(TILES_DEV)]
    hub_row_block, hub_col_block = mark(IDS + 2 * TILES_DEV), mark(IDS + 2 * TILES_DEV + 1)

    def degrees_of(block):
        return jnp.concatenate([degrees_a[stored(block)], degrees_b[block]], axis=0)

    def out_copy(q):
        return pltpu.make_async_copy(
            staged.at[q], owned_ref.at[q // 2, pl.ds(CHUNK * (q % 2), CHUNK)], out_sem.at[q]
        )

    def product(b, q):
        def line(f):
            return jnp.concatenate(
                [fields[f, pl.ds(2 * b + i, 1), :] for i in range(2 * SPAN)], axis=1
            )

        left = weighted(one_hot(line(0) - 256.0 * q, CHUNK), line(3))
        right = jnp.concatenate(
            [ones_where(one_hot(line(1), 256)), ones_where(one_hot(line(2), 256))], axis=0
        )
        return lax.dot_general(left, right, NT, preferred_element_type=F32)

    firsts = [starts[q] >> 8 for q in range(CHUNKS)]

    def add_rest(q):
        def add_blocks(i, _):
            total[q % 2] += product(firsts[q] + SPAN * i, q)
            return 0

        blocks = ((starts[q + 1] + 255) >> 8) - firsts[q]
        lax.fori_loop(1, (blocks + SPAN - 1) // SPAN, add_blocks, 0)

    def hub_product(b):
        def line(f):
            return jnp.concatenate(
                [hub_fields[f, pl.ds(HUB_SPAN * b + i, 1), :] for i in range(HUB_SPAN)], axis=1
            )

        return lax.dot_general(
            weighted(one_hot(line(0), LANES), line(2)), ones_where(one_hot(line(1), 256)),
            NT, preferred_element_type=F32,
        )

    scaling = jnp.sum(degrees_a[...], axis=0) + jnp.sum(degrees_b[...], axis=0)
    scaling = jnp.sum(scaling) / (N_ROW * N_COL * TILE)
    gathered[...] = jnp.ones_like(gathered)
    for t in range(TILES_DEV):
        gathered[pl.ds(4 * t, 4), :] = degrees_of(row_blocks[t])
    gathered[pl.ds(24, 4), :] = degrees_of(hub_row_block)
    hub_row = gathered[pl.ds(24 + lax.rem(col, 8) // 2, 1), :]
    gathered[pl.ds(16, 8), :] = pltpu.roll(
        jnp.broadcast_to(hub_row, (8, LANES)), 64 * lax.rem(col, 2), axis=1
    )
    degree_rows = (scaling / gathered[...]).T

    total[0] = product(0, 0)
    hub_total[...] = hub_product(0)
    add_rest(0)

    def add_hub(b, _):
        hub_total[...] += hub_product(b)
        return 0

    lax.fori_loop(1, used, add_hub, 0)
    hub_degree = 1.0 / degrees_of(hub_col_block)
    for n in range(4):
        values = hub_total[pl.ds(64 * (n // 2), 64), pl.ds(LANES * (n % 2), LANES)]
        values = values * degree_rows[0:64, 16:17] * hub_degree[n : n + 1]
        hub_ref[:, pl.ds(LANES * n, LANES)] = jnp.log(jnp.maximum(values, 1.0))
    hub_copy = pltpu.make_async_copy(hub_ref, hub_out, out_sem.at[CHUNKS])
    hub_copy.start()

    for q in range(CHUNKS):
        if q + 1 < CHUNKS:
            total[(q + 1) % 2] = product(firsts[q + 1], q + 1)
        tile = q // 2
        degree = 1.0 / degrees_of(col_blocks[tile])
        for j in range(2):
            rows = degree_rows[:, 4 * tile + 2 * (q % 2) + j][:, None]
            for n in range(4):
                values = total[q % 2, pl.ds(LANES * j, LANES), pl.ds(LANES * n, LANES)]
                values = values * rows * degree[n : n + 1]
                staged[q, pl.ds(LANES * j, LANES), pl.ds(LANES * n, LANES)] = jnp.log(
                    jnp.maximum(values, 1.0)
                )
        out_copy(q).start()
        if q + 1 < CHUNKS:
            add_rest(q + 1)

    flag_copy.wait()
    hub_copy.wait()
    for q in range(CHUNKS):
        out_copy(q).wait()


def tiles(*arranged):
    vmem = pl.BlockSpec(memory_space=pltpu.VMEM)
    hbm = pl.BlockSpec(memory_space=pltpu.HBM)
    return pl.pallas_call(
        tile_kernel,
        out_shape=(
            jax.ShapeDtypeStruct((TILES_DEV, TILE, TILE), F32),
            jax.ShapeDtypeStruct((HUBS * TILE // N_COL, TILE), F32),
            jax.ShapeDtypeStruct((1, 1), jnp.int32),
        ),
        in_specs=[vmem] * 5,
        out_specs=(hbm, hbm, hbm),
        scratch_shapes=[
            pltpu.SMEM((1, 1), jnp.int32),
            pltpu.VMEM((2, CHUNK, TILE), F32),
            pltpu.VMEM((LANES, 256), F32),
            pltpu.VMEM((CHUNKS, CHUNK, TILE), F32),
            pltpu.VMEM((HUBS * TILE // N_COL, TILE), F32),
            pltpu.VMEM((LANES, LANES), F32),
            pltpu.SemaphoreType.DMA((CHUNKS + 1,)),
            pltpu.SemaphoreType.DMA(()),
        ],
        compiler_params=pltpu.CompilerParams(vmem_limit_bytes=32 << 20),
    )(*arranged)


def dense_hub(code, weight, count, hubs, degree):
    def to_owner(x):
        return lax.all_to_all(
            x.reshape(N_ROW * N_COL, -1), ("row", "col"), split_axis=0, concat_axis=0, tiled=True
        )

    codes, weights, counts = to_owner(code), to_owner(weight), to_owner(count)
    usable = jnp.arange(CAP, dtype=jnp.int32)[None, :] < counts
    weights = jnp.where(usable, weights, jnp.zeros((), BF16)).reshape(-1)
    codes = codes.reshape(-1) - TILES_DEV * TILE * TILE

    def step(turn, sums):
        part = lax.dynamic_slice_in_dim(codes, turn * 512, 512)
        value = lax.dynamic_slice_in_dim(weights, turn * 512, 512)
        left = jnp.where(
            (part >> 9)[:, None] == jnp.arange(HUBS * TILE, dtype=jnp.int32)[None, :],
            value[:, None], jnp.zeros((), BF16),
        )
        right = ((part & 511)[:, None] == jnp.arange(TILE, dtype=jnp.int32)[None, :]).astype(BF16)
        return sums + lax.dot_general(
            left, right, (((0,), (0,)), ((), ())), preferred_element_type=F32
        )

    sums = lax.fori_loop(
        0, codes.shape[0] // 512, step, jnp.zeros((HUBS * TILE, TILE), F32)
    )
    sums = sums.reshape(N_COL, HUBS * TILE // N_COL, TILE)
    sums = jnp.sum(lax.all_to_all(sums, "col", 0, 0, tiled=True), axis=0)
    slab_rows = HUBS * TILE // N_COL
    offset = lax.axis_index("col") * slab_rows
    degrees = to_owner(jnp.broadcast_to(degree, (N_ROW * N_COL, TILE)))
    scaling = jnp.mean(degrees)
    pair = lax.dynamic_index_in_dim(hubs[0], offset // TILE, 0, keepdims=False)
    row_degree = lax.dynamic_index_in_dim(degrees, pair[0], 0, keepdims=False)
    row_degree = lax.dynamic_slice_in_dim(row_degree, lax.rem(offset, TILE), slab_rows)
    col_degree = lax.dynamic_index_in_dim(degrees, pair[1], 0, keepdims=False)
    return jnp.log(
        jnp.maximum(scaling * sums / (row_degree[:, None] * col_degree[None, :]), 1.0)
    )


def in_hbm(x):
    return pltpu.with_memory_space_constraint(x, pltpu.HBM)


def shards(edge_code, edge_weight, edge_count, tile_blocks, hub_blocks, node_degree):
    fields, hub_fields, marks, degrees_a, degrees_b = exchange(
        in_hbm(edge_code.reshape(32, LANES)), in_hbm(edge_weight), in_hbm(edge_count),
        in_hbm(node_degree.reshape(2, 2, LANES)), in_hbm(tile_blocks.transpose(0, 2, 1)),
        in_hbm(hub_blocks),
    )
    degrees_a, degrees_b = (x.reshape(-1, 2, LANES) for x in (degrees_a, degrees_b))
    owned, hub, crowded = tiles(fields, hub_fields, marks, degrees_a, degrees_b)
    def dense(_):
        hub = dense_hub(edge_code, edge_weight, edge_count, hub_blocks, node_degree)
        return jnp.zeros_like(crowded), hub

    _, hub = lax.while_loop(lambda state: state[0][0, 0] > 0, dense, (crowded, hub))
    return owned, hub


def solution(mesh):
    both = ("row", "col")
    return jax.shard_map(
        shards,
        mesh=mesh,
        in_specs=(
            P(both, None), P(both, None), P(both, None),
            P(both, None, None), P("row", None, None), P(both, None),
        ),
        out_specs=(P(both, None, None), P(both, None)),
        check_vma=False,
    )
```
